8 devices in a mesh: nodes: 8 (over z, y, x, core).
Axes of the slice: x: 2, y: 2, z: 1, core: 2. Of those that a mesh axis runs over, the one named last changes fastest.
Arguments:
- adjacency: bfloat16 [16384, 16384], P('nodes')
- features: bfloat16 [16384, 128], P('nodes')
- w_one: float32 [128, 256], replicated
- w_two: float32 [256, 40], replicated
- labels: int32 [16384], P('nodes')
- label_mask: int32 [16384], P('nodes')
Outputs:
- output 1: float32 [1], replicated
- output 2: float32 [128, 256], replicated
- output 3: float32 [256, 40], replicated
All inputs are finite; a program needn't handle non-finite values.
Results may differ from the reference program's by a relative error of at most 0.001.
Values are sent between devices in bfloat16 or wider.
A program may use at most 1 GiB of HBM per device.

```python
import math
import jax
import jax.numpy as jnp
from jax import lax

NODES = 16384
BLOCK_ROWS = 2048
F_IN = 128
HIDDEN = 256
CLASSES = 40

ROW_CONTRACT = (((0,), (0,)), ((), ()))
COL_CONTRACT = (((1,), (1,)), ((), ()))


def setup_inputs(seed: int = 0) -> dict:
    key_list = jax.random.split(jax.random.key(seed), 8)
    num_comms = NODES // BLOCK_ROWS
    shifts = jax.random.randint(key_list[0], (2,), 1, num_comms)
    col_ids = jnp.arange(NODES)
    col_comm = col_ids // BLOCK_ROWS
    row_ids = jnp.arange(BLOCK_ROWS)

    def draw_rows(block_idx):
        hot_cols = (col_comm == (block_idx + shifts[0]) % num_comms) | (col_comm == (block_idx + shifts[1]) % num_comms)
        edge_prob = jnp.where(hot_cols, 0.5, 0.01)
        coin_flip = jax.random.uniform(jax.random.fold_in(key_list[1], block_idx), (BLOCK_ROWS, NODES))
        self_loop = col_ids[None, :] == block_idx * BLOCK_ROWS + row_ids[:, None]
        raw_edges = jnp.where((coin_flip < edge_prob[None, :]) | self_loop, 1.0, 0.0)
        return (raw_edges / jnp.sum(raw_edges, axis=1, keepdims=True)).astype(jnp.bfloat16)

    adjacency = lax.map(draw_rows, jnp.arange(num_comms)).reshape(NODES, NODES)
    centers = jax.random.normal(key_list[2], (num_comms, F_IN))
    feat_noise = jax.random.normal(key_list[3], (NODES, F_IN))
    features = (jnp.repeat(centers, BLOCK_ROWS, axis=0) + feat_noise).astype(jnp.bfloat16)
    w_one = jax.random.normal(key_list[4], (F_IN, HIDDEN)) * math.sqrt(2.0 / F_IN)
    w_two = jax.random.normal(key_list[5], (HIDDEN, CLASSES)) * (2.0 / math.sqrt(HIDDEN))
    labels = jax.random.randint(key_list[6], (NODES,), 0, CLASSES, dtype=jnp.int32)
    drawn_mask = jax.random.randint(key_list[7], (NODES,), 0, 10, dtype=jnp.int32) < 3
    label_mask = jnp.where((jnp.arange(NODES) % 10 == 0) | drawn_mask, 1, 0).astype(jnp.int32)
    return {'adjacency': adjacency, 'features': features, 'w_one': w_one.astype(jnp.float32), 'w_two': w_two.astype(jnp.float32), 'labels': labels, 'label_mask': label_mask}


def reference(adjacency, features, w_one, w_two, labels, label_mask):
    weight_one = w_one.astype(jnp.bfloat16)
    weight_two = w_two.astype(jnp.bfloat16)
    agg_one = jnp.dot(adjacency, features, preferred_element_type=jnp.float32).astype(jnp.bfloat16)
    pre_one = jnp.dot(agg_one, weight_one, preferred_element_type=jnp.float32)
    hidden = jnp.maximum(pre_one, 0.0).astype(jnp.bfloat16)
    agg_two = jnp.dot(adjacency, hidden, preferred_element_type=jnp.float32).astype(jnp.bfloat16)
    logits = jnp.dot(agg_two, weight_two, preferred_element_type=jnp.float32)
    weight = label_mask.astype(jnp.float32)
    label_count = jnp.sum(weight)
    onehot = (labels[:, None] == jnp.arange(CLASSES)[None, :]).astype(jnp.float32)
    log_prob = jax.nn.log_softmax(logits, axis=-1)
    loss_value = -jnp.sum(weight * jnp.sum(onehot * log_prob, axis=-1)) / label_count
    grad_two = (weight[:, None] * (jnp.exp(log_prob) - onehot) / label_count).astype(jnp.bfloat16)
    dw_two = lax.dot_general(agg_two, grad_two, ROW_CONTRACT, preferred_element_type=jnp.float32)
    back_two = lax.dot_general(grad_two, weight_two, COL_CONTRACT, preferred_element_type=jnp.float32).astype(jnp.bfloat16)
    d_hidden = lax.dot_general(adjacency, back_two, ROW_CONTRACT, preferred_element_type=jnp.float32)
    grad_one = jnp.where(pre_one > 0.0, d_hidden, 0.0).astype(jnp.bfloat16)
    dw_one = lax.dot_general(agg_one, grad_one, ROW_CONTRACT, preferred_element_type=jnp.float32)
    return (loss_value.reshape(1), dw_one, dw_two)
```

```python
import functools

import jax
import jax.numpy as jnp
from jax import lax
from jax.experimental import pallas as pl
from jax.experimental.pallas import tpu as pltpu
from jax.sharding import PartitionSpec as P

AXIS = "nodes"
MESH = pl.DeviceIdType.MESH
F32 = jnp.float32
BF16 = jnp.bfloat16

SLOTS = 3
M_CHUNK = 512


def _dot(a, b):
    return jnp.dot(a, b, preferred_element_type=F32)


def _dot_nt(a, b):
    return lax.dot_general(a, b, (((1,), (1,)), ((), ())), preferred_element_type=F32)


def _kernel(
    adj, feat, w_one, w_two, labels, mask,
    out_loss, out_one, out_two,
    feats_all, aggs_all, hid, acc_one, acc_two, agg_two, back_t, grad_t, pre_t,
    own_sums, stage, from_pair, from_chip, adj_ring,
    w_one_f, w_two_f, w_one_b, w_one_t, w_two_b, w_two_t, lab_v, mask_v, count, count_in,
    red, red_pair, red_link, red_next, red_last, red_out,
    adj_sem, load_sem, gather_send, gather_recv, count_send, count_recv,
    pair_send, pair_recv, chip_send, chip_recv, red_send, red_recv,
):
    rows = feat.shape[0]
    half_rows, quarter = rows // 2, rows // 4
    classes = w_two.shape[1]
    me = lax.axis_index(AXIS)
    core, chip_x, chip_y = lax.rem(me, 2), lax.rem(me // 2, 2), me // 4
    to_pair, to_x, to_y = 1 - 2 * core, 2 - 4 * chip_x, 4 - 8 * chip_y
    pair, x_next, y_next = me + to_pair, me + to_x, me + to_y

    def remote(src, dst, send, recv, dev):
        return pltpu.make_async_remote_copy(
            src_ref=src, dst_ref=dst, send_sem=send, recv_sem=recv, device_id=(dev,), device_id_type=MESH)

    def gather_place(s):
        flip = lax.rem(s // 2, 2)
        far = s // 12
        near = (s + 12) // 16 - far
        along_y = lax.rem(s, 2)
        second = (s // 8) * (1 - far)
        blk = me + flip * to_pair + (near * (1 - along_y) + far) * to_x + (near * along_y + far) * to_y
        return blk, lax.rem(s + second, 2)

    def reduce_place(u):
        own = u // 12
        diag = 1 - (u + 12) // 16
        link = lax.rem(u, 2)
        nx = (1 - own) * (diag + (1 - diag) * (1 - link))
        ny = (1 - own) * (diag + (1 - diag) * link)
        part = own * (u - 12) + (1 - own) * (2 * lax.rem(link + u // 8, 2) + lax.rem(u // 2, 2))
        return me + nx * to_x + ny * to_y, part

    def slab_copy(n):
        blk, half = gather_place(lax.rem(n, 16))
        col = pl.multiple_of(blk * rows + half * half_rows, half_rows)
        slot = lax.rem(n, SLOTS)
        return pltpu.make_async_copy(adj.at[:, pl.ds(col, half_rows)], adj_ring.at[slot], adj_sem.at[slot, 0])

    def part_copy(n, which):
        blk, part = reduce_place(n - 32)
        blk = blk + to_pair * (1 - which)
        col = pl.multiple_of(blk * rows + part * quarter, quarter)
        slot = lax.rem(n, SLOTS)
        return pltpu.make_async_copy(
            adj.at[:, pl.ds(col, quarter)],
            adj_ring.at[slot, :, pl.ds(which * quarter, quarter)], adj_sem.at[slot, which])

    def fetch(n):
        @pl.when(n < 32)
        def _():
            slab_copy(n).start()

        @pl.when((n >= 32) & (n < 48))
        def _():
            part_copy(n, 0).start()
            part_copy(n, 1).start()

    loads = [
        pltpu.make_async_copy(feat, feats_all.at[me], load_sem.at[0]),
        pltpu.make_async_copy(mask, mask_v, load_sem.at[1]),
        pltpu.make_async_copy(w_one, w_one_f, load_sem.at[2]),
        pltpu.make_async_copy(w_two, w_two_f, load_sem.at[3]),
        pltpu.make_async_copy(labels, lab_v, load_sem.at[4]),
    ]
    for load in loads:
        load.start()
    for n in range(SLOTS):
        slab_copy(n).start()

    barrier = pltpu.get_barrier_semaphore()
    for dev in (pair, x_next, y_next):
        pl.semaphore_signal(barrier, inc=1, device_id=(dev,), device_id_type=MESH)
    acc_one[...] = jnp.zeros_like(acc_one)
    acc_two[...] = jnp.zeros_like(acc_two)
    grad_t[...] = jnp.zeros_like(grad_t)
    pl.semaphore_wait(barrier, 3)

    def piece(buf, s):
        blk, half = gather_place(s)
        return buf.at[blk, pl.ds(pl.multiple_of(half * half_rows, half_rows), half_rows), :]

    def send_piece(ph, buf, s, to, dev):
        ref = piece(buf, s)
        return remote(ref, ref, gather_send.at[ph, to], gather_recv.at[ph, to], dev)

    def send_own(ph, buf, half):
        send_piece(ph, buf, half, 4 + 4 * half, x_next).start()
        send_piece(ph, buf, half, 9 - 4 * half, y_next).start()

    def gather_step(ph, buf, s):
        @pl.when(s >= 2)
        def _():
            send_piece(ph, buf, s, s, pair).wait_recv()

        @pl.when(s == 4)
        def _():
            send_piece(ph, buf, 4, 12, y_next).start()

        @pl.when(s == 5)
        def _():
            send_piece(ph, buf, 5, 13, x_next).start()

        @pl.when(lax.rem(s // 2, 2) == 0)
        def _():
            send_piece(ph, buf, s, s + 2, pair).start()

    def count_move(i):
        return remote(count.at[i], count_in.at[i], count_send.at[i], count_recv.at[i], (pair, x_next, y_next)[i])

    loads[0].wait()
    send_piece(0, feats_all, 0, 4, x_next).start()
    send_piece(0, feats_all, 1, 5, y_next).start()
    send_piece(0, feats_all, 1, 8, x_next).start()
    send_piece(0, feats_all, 0, 9, y_next).start()
    for load in loads[1:]:
        load.wait()
    count[0] = jnp.full((8, 128), jnp.sum(mask_v[...].astype(F32)), F32)
    count_move(0).start()
    w_one_b[...] = w_one_f[...].astype(BF16)
    w_one_t[...] = w_one_f[...].T.astype(BF16)
    w_two_b[...] = jnp.zeros_like(w_two_b)
    w_two_b[:, :classes] = w_two_f[...].astype(BF16)
    w_two_t[...] = w_two_b[...].astype(F32).T.astype(BF16)

    def step_one(s, carry):
        gather_step(0, feats_all, s)

        for i, when in enumerate((1, 12)):
            @pl.when(s == when)
            def _(i=i):
                count_move(i).wait_recv()
                count[i + 1] = count[i] + count_in[i]
                count_move(i + 1).start()

        slab_copy(s).wait()
        slot = lax.rem(s, SLOTS)
        right = piece(feats_all, s)[...]
        for m in range(0, rows, M_CHUNK):
            at = pl.ds(m, M_CHUNK)
            acc_one[at, :] += _dot(adj_ring[slot, at, :], right)
        fetch(s + SLOTS)
        return carry

    lax.fori_loop(0, 16, step_one, 0)

    aggs_all[me] = acc_one[...].astype(BF16)
    send_piece(1, aggs_all, 0, 4, x_next).start()
    send_piece(1, aggs_all, 1, 5, y_next).start()
    send_piece(1, aggs_all, 1, 8, x_next).start()
    send_piece(1, aggs_all, 0, 9, y_next).start()

    def step_two(s, carry):
        gather_step(1, aggs_all, s)
        hid[...] = jnp.maximum(_dot(piece(aggs_all, s)[...], w_one_b[...]), 0.0).astype(BF16)
        n = s + 16
        slab_copy(n).wait()
        slot = lax.rem(n, SLOTS)
        right = hid[...]
        for m in range(0, rows, M_CHUNK):
            at = pl.ds(m, M_CHUNK)
            acc_two[at, :] += _dot(adj_ring[slot, at, :], right)
        fetch(n + SLOTS)
        return carry

    lax.fori_loop(0, 16, step_two, 0)

    count_move(2).wait_recv()
    total = (count[2] + count_in[2])[0:1, 0:1]
    agg_two[...] = acc_two[...].astype(BF16)
    logits = _dot_nt(w_two_t[0:48, :], agg_two[...])[:classes, :]
    weight = mask_v[...].astype(F32)
    shifted = logits - jnp.max(logits, axis=0, keepdims=True)
    log_prob = shifted - jnp.log(jnp.sum(jnp.exp(shifted), axis=0, keepdims=True))
    onehot = (lax.broadcasted_iota(jnp.int32, (classes, rows), 0) == lab_v[...]).astype(F32)
    picked = jnp.sum(onehot * log_prob, axis=0, keepdims=True)
    loss_sum = -jnp.sum(weight * picked)
    grad_t[:classes, :] = (weight * (jnp.exp(log_prob) - onehot) / total).astype(BF16)
    back_t[...] = _dot(w_two_b[...], grad_t[...]).astype(BF16)

    def pair_move(u):
        return remote(stage.at[lax.rem(u, 4)], from_pair.at[u], pair_send.at[lax.rem(u, 4)], pair_recv.at[u], pair)

    def chip_move(u):
        link = lax.rem(u, 2)
        dev = me + (1 - link) * to_x + link * to_y
        return remote(own_sums.at[u], from_chip.at[link, u // 2], chip_send.at[u], chip_recv.at[link, u // 2], dev)

    def finish(u):
        pair_move(u).wait_recv()
        own_sums[u] += from_pair[u]

        @pl.when(u < 8)
        def _():
            chip_move(u).start()

    def step_three(u, carry):
        n = u + 32
        slot = lax.rem(n, SLOTS)

        @pl.when(u >= 4)
        def _():
            pair_move(u).wait_send()

        part_copy(n, 0).wait()
        stage[lax.rem(u, 4)] = _dot(back_t[...], adj_ring[slot, :, pl.ds(0, quarter)])
        pair_move(u).start()
        part_copy(n, 1).wait()
        own_sums[u] = _dot(back_t[...], adj_ring[slot, :, pl.ds(quarter, quarter)])
        fetch(n + SLOTS)

        @pl.when(u >= 1)
        def _():
            finish(u - 1)

        return carry

    lax.fori_loop(0, 16, step_three, 0)
    finish(jnp.int32(15))
    for u in range(12, 16):
        pair_move(u).wait_send()

    part_two = _dot(grad_t[0:48, :], agg_two[...])
    red[256:296, :] = part_two[0:classes, 0:128]
    red[296:336, :] = part_two[0:classes, 128:256]
    red[336:352, :] = jnp.full((16, 128), loss_sum, F32)
    pre_t[...] = _dot_nt(w_one_t[...], aggs_all[me])

    for k in range(2):
        for link in range(2):
            u = 8 + 2 * k + (1 - link)
            chip_move(2 * k + link).wait_recv()
            own_sums[u] += from_chip[link, k]
            chip_move(u).start()

    def part_of_one(j):
        return 12 + j

    for k in range(2):
        for link in range(2):
            j = 2 * link + k
            chip_move(4 + 2 * k + link).wait_recv()
            own_sums[12 + j] += from_chip[link, 2 + k]
    red_one = jnp.zeros((256, 128), F32)
    for k in range(2):
        for link in range(2):
            j = 2 * (1 - link) + k
            chip_move(8 + 2 * k + link).wait_recv()
            d_hidden = own_sums[12 + j] + from_chip[link, 4 + k]
            keep = pre_t[:, pl.ds(j * quarter, quarter)] > 0.0
            grad_one = jnp.where(keep, d_hidden, 0.0).astype(BF16)
            red_one += _dot(grad_one, aggs_all[me, pl.ds(j * quarter, quarter), :])
    red[0:256, :] = red_one

    n_half = red.shape[0] // 2
    n_part = n_half // 2
    mine = pl.multiple_of(core * n_half, 8)
    other = pl.multiple_of((1 - core) * n_half, 8)

    move = remote(red.at[pl.ds(other, n_half)], red_pair, red_send.at[0], red_recv.at[0], pair)
    move.start()
    move.wait_recv()
    red_link[...] = red[pl.ds(mine, n_half), :] + red_pair[...]
    moves = [
        remote(red_link.at[pl.ds(i * n_part, n_part)], red_next.at[pl.ds(i * n_part, n_part)],
               red_send.at[1 + i], red_recv.at[1 + i], (x_next, y_next)[i])
        for i in range(2)
    ]
    for m in moves:
        m.start()
    for m in moves:
        m.wait_recv()
    red_pair2 = red_link[...] + red_next[...]
    red_last[0] = red_pair2
    lasts = [
        remote(red_last.at[0, pl.ds(i * n_part, n_part)], red_last.at[1, pl.ds(i * n_part, n_part)],
               red_send.at[3 + i], red_recv.at[3 + i], (y_next, x_next)[i])
        for i in range(2)
    ]
    for m in lasts:
        m.start()
    for m in lasts:
        m.wait_recv()
    red_out[pl.ds(mine, n_half), :] = red_last[0] + red_last[1]
    ref = red_out.at[pl.ds(mine, n_half)]
    back = remote(ref, ref, red_send.at[5], red_recv.at[5], pair)
    back.start()
    ref_in = red_out.at[pl.ds(other, n_half)]
    remote(ref_in, ref_in, red_send.at[5], red_recv.at[5], pair).wait_recv()

    out_one[...] = red_out[0:256, :].T
    out_two[0:128, :] = red_out[256:296, :].T
    out_two[128:256, :] = red_out[296:336, :].T
    out_loss[...] = red_out[336:337, 0:1] / total

    move.wait_send()
    for m in moves + lasts + [back]:
        m.wait_send()
    for i in range(3):
        count_move(i).wait_send()
    for ph, buf in ((0, feats_all), (1, aggs_all)):
        for to in range(2, 16):
            send_piece(ph, buf, to, to, pair).wait_send()
    for u in range(12):
        chip_move(u).wait_send()


def solution(mesh):
    def step(adj, feat, w_one, w_two, labels, mask):
        rows, nodes = adj.shape
        feat_dim, hidden = w_one.shape
        classes = w_two.shape[1]
        parts = nodes // rows
        any_spec = pl.BlockSpec(memory_space=pltpu.HBM)
        vmem = pl.BlockSpec(memory_space=pltpu.VMEM)
        quarter = rows // 4
        scratch = [
            pltpu.VMEM((parts, rows, feat_dim), BF16),
            pltpu.VMEM((parts, rows, feat_dim), BF16),
            pltpu.VMEM((rows // 2, hidden), BF16),
            pltpu.VMEM((rows, feat_dim), F32),
            pltpu.VMEM((rows, hidden), F32),
            pltpu.VMEM((rows, hidden), BF16),
            pltpu.VMEM((hidden, rows), BF16),
            pltpu.VMEM((128, rows), BF16),
            pltpu.VMEM((hidden, rows), F32),
            pltpu.VMEM((16, hidden, quarter), F32),
            pltpu.VMEM((4, hidden, quarter), F32),
            pltpu.VMEM((16, hidden, quarter), F32),
            pltpu.VMEM((2, 6, hidden, quarter), F32),
            pltpu.VMEM((SLOTS, rows, rows // 2), BF16),
            pltpu.VMEM((feat_dim, hidden), F32),
            pltpu.VMEM((hidden, classes), F32),
            pltpu.VMEM((feat_dim, hidden), BF16),
            pltpu.VMEM((hidden, feat_dim), BF16),
            pltpu.VMEM((hidden, 128), BF16),
            pltpu.VMEM((128, hidden), BF16),
            pltpu.VMEM((1, rows), jnp.int32),
            pltpu.VMEM((1, rows), jnp.int32),
            pltpu.VMEM((3, 8, 128), F32),
            pltpu.VMEM((3, 8, 128), F32),
            pltpu.VMEM((352, 128), F32),
            pltpu.VMEM((176, 128), F32),
            pltpu.VMEM((176, 128), F32),
            pltpu.VMEM((176, 128), F32),
            pltpu.VMEM((2, 176, 128), F32),
            pltpu.VMEM((352, 128), F32),
            pltpu.SemaphoreType.DMA((SLOTS, 2)),
            pltpu.SemaphoreType.DMA((5,)),
            pltpu.SemaphoreType.DMA((2, 16)),
            pltpu.SemaphoreType.DMA((2, 16)),
            pltpu.SemaphoreType.DMA((3,)),
            pltpu.SemaphoreType.DMA((3,)),
            pltpu.SemaphoreType.DMA((4,)),
            pltpu.SemaphoreType.DMA((16,)),
            pltpu.SemaphoreType.DMA((12,)),
            pltpu.SemaphoreType.DMA((2, 6)),
            pltpu.SemaphoreType.DMA((6,)),
            pltpu.SemaphoreType.DMA((6,)),
        ]
        loss, dw_one, dw_two = pl.pallas_call(
            _kernel,
            out_shape=(
                jax.ShapeDtypeStruct((1, 1), F32),
                jax.ShapeDtypeStruct((feat_dim, hidden), F32),
                jax.ShapeDtypeStruct((hidden, classes), F32),
            ),
            in_specs=[any_spec] * 6,
            out_specs=(vmem, vmem, vmem),
            scratch_shapes=scratch,
            compiler_params=pltpu.CompilerParams(
                collective_id=0, has_side_effects=True, vmem_limit_bytes=67_000_000),
            name="gcn_step",
        )(adj, feat, w_one, w_two, labels.reshape(1, rows), mask.reshape(1, rows))
        return loss.reshape(1), dw_one, dw_two

    return jax.shard_map(
        step,
        mesh=mesh,
        in_specs=(P(AXIS, None), P(AXIS, None), P(None, None), P(None, None), P(AXIS), P(AXIS)),
        out_specs=(P(None), P(None, None), P(None, None)),
        check_vma=False,
    )
```

```python
import functools

import jax
import jax.numpy as jnp
from jax import lax
from jax.experimental import pallas as pl
from jax.experimental.pallas import tpu as pltpu
from jax.sharding import PartitionSpec as P

AXIS = "nodes"
MESH = pl.DeviceIdType.MESH
F32 = jnp.float32
BF16 = jnp.bfloat16

SLOTS = 3
M_CHUNK = 512


def _dot(a, b):
    return jnp.dot(a, b, preferred_element_type=F32)


def _dot_nt(a, b):
    return lax.dot_general(a, b, (((1,), (1,)), ((), ())), preferred_element_type=F32)


def _kernel(
    adj, feat, w_one, w_two, labels, mask,
    out,
    feats_all, aggs_all, hid, acc_one, acc_two, agg_two, back_t, grad_t, pre_t,
    own_sums, stage, from_pair, from_chip, adj_ring,
    w_one_f, w_two_f, w_one_b, w_one_t, w_two_b, w_two_t, lab_v, mask_v, count, count_in,
    red, red_pair, red_link, red_next, red_last, red_out, small, small_in,
    adj_sem, load_sem, gather_send, gather_recv, count_send, count_recv,
    pair_send, pair_recv, chip_send, chip_recv, red_send, red_recv, small_send, small_recv,
):
    rows = feat.shape[0]
    quarter = rows // 4
    classes = w_two.shape[0]
    me = lax.axis_index(AXIS)
    core, chip_x, chip_y = lax.rem(me, 2), lax.rem(me // 2, 2), me // 4
    to_pair, to_x, to_y = 1 - 2 * core, 2 - 4 * chip_x, 4 - 8 * chip_y
    pair, x_next, y_next = me + to_pair, me + to_x, me + to_y

    def remote(src, dst, send, recv, dev):
        return pltpu.make_async_remote_copy(
            src_ref=src, dst_ref=dst, send_sem=send, recv_sem=recv, device_id=(dev,), device_id_type=MESH)

    def gather_place(s, e):
        low = 1 - (s + 12) // 16
        far = s // 12
        near = 1 - low - far
        flip = low * (s // 2) + (1 - low) * lax.rem(s, 2)
        blk = me + flip * to_pair + (near * (1 - e) + far) * to_x + (near * e + far) * to_y
        part = (low * (2 * lax.rem(s, 2) + e) + near * lax.rem(s // 2 + 2 + 2 * e, 4) + far * (s // 2 - 6 + 2 * e))
        return blk, part

    def reduce_place(u):
        own = u // 12
        diag = 1 - (u + 12) // 16
        link = lax.rem(u, 2)
        nx = (1 - own) * (diag + (1 - diag) * (1 - link))
        ny = (1 - own) * (diag + (1 - diag) * link)
        part = own * (u - 12) + (1 - own) * (2 * lax.rem(link + u // 8, 2) + lax.rem(u // 2, 2))
        return me + nx * to_x + ny * to_y, part

    def adj_copy(place, n, e):
        blk, part = place
        col = pl.multiple_of(blk * rows + part * quarter, quarter)
        slot = lax.rem(n, SLOTS)
        return pltpu.make_async_copy(
            adj.at[:, pl.ds(col, quarter)], adj_ring.at[slot, :, pl.ds(e * quarter, quarter)], adj_sem.at[slot, e])

    def slab_copy(n, e):
        return adj_copy(gather_place(lax.rem(n, 16), e), n, e)

    def part_copy(n, e):
        blk, part = reduce_place(n - 32)
        return adj_copy((blk + to_pair * (1 - e), part), n, e)

    def fetch(n):
        @pl.when(n < 32)
        def _():
            for e in range(2):
                slab_copy(n, e).start()

        @pl.when((n >= 32) & (n < 48))
        def _():
            for e in range(2):
                part_copy(n, e).start()

    loads = [
        pltpu.make_async_copy(feat, feats_all.at[me], load_sem.at[0]),
        pltpu.make_async_copy(mask, mask_v, load_sem.at[1]),
        pltpu.make_async_copy(w_one, w_one_f, load_sem.at[2]),
        pltpu.make_async_copy(w_two, w_two_f, load_sem.at[3]),
        pltpu.make_async_copy(labels, lab_v, load_sem.at[4]),
    ]
    for load in loads:
        load.start()
    for n in range(SLOTS):
        for e in range(2):
            slab_copy(n, e).start()

    barrier = pltpu.get_barrier_semaphore()
    for dev in (pair, x_next, y_next):
        pl.semaphore_signal(barrier, inc=1, device_id=(dev,), device_id_type=MESH)
    acc_one[...] = jnp.zeros_like(acc_one)
    acc_two[...] = jnp.zeros_like(acc_two)
    grad_t[...] = jnp.zeros_like(grad_t)
    pl.semaphore_wait(barrier, 3)

    def piece(buf, s, e):
        blk, part = gather_place(s, e)
        return buf.at[blk, pl.ds(pl.multiple_of(part * quarter, quarter), quarter), :]

    def send_piece(ph, buf, s, e, to, dev):
        ref = piece(buf, s, e)
        at = 2 * to + e
        return remote(ref, ref, gather_send.at[ph, at], gather_recv.at[ph, at], dev)

    def send_own(ph, buf):
        for i in range(4):
            for e, dev in ((0, x_next), (1, y_next)):
                part = (i + 2 * e) % 4
                ref = buf.at[me, pl.ds(part * quarter, quarter), :]
                at = 2 * (4 + 2 * i) + e
                remote(ref, ref, gather_send.at[ph, at], gather_recv.at[ph, at], dev).start()

    def gather_step(ph, buf, s):
        for e in range(2):
            @pl.when(s >= 2)
            def _():
                send_piece(ph, buf, s, e, s, pair).wait_recv()

            @pl.when((s == 4) | (s == 6))
            def _():
                send_piece(ph, buf, s, e, s + 8, (y_next, x_next)[e]).start()

            @pl.when(s < 2)
            def _():
                send_piece(ph, buf, s, e, s + 2, pair).start()

            @pl.when((s >= 4) & (lax.rem(s, 2) == 0))
            def _():
                send_piece(ph, buf, s, e, s + 1, pair).start()

    def count_move(i):
        return remote(count.at[i], count_in.at[i], count_send.at[i], count_recv.at[i], (pair, x_next, y_next)[i])

    loads[0].wait()
    send_own(0, feats_all)
    for load in loads[1:]:
        load.wait()
    count[0] = jnp.full((8, 128), jnp.sum(mask_v[...].astype(F32)), F32)
    count_move(0).start()
    w_one_b[...] = w_one_f[...].astype(BF16)
    w_one_t[...] = w_one_f[...].T.astype(BF16)
    w_two_t[...] = jnp.zeros_like(w_two_t)
    w_two_t[:classes, :] = w_two_f[...].astype(BF16)
    w_two_b[...] = w_two_t[...].astype(F32).T.astype(BF16)

    def step_one(s, carry):
        gather_step(0, feats_all, s)

        for i, when in enumerate((1, 12)):
            @pl.when(s == when)
            def _(i=i):
                count_move(i).wait_recv()
                count[i + 1] = count[i] + count_in[i]
                count_move(i + 1).start()

        for e in range(2):
            slab_copy(s, e).wait()
        slot = lax.rem(s, SLOTS)
        right = jnp.concatenate([piece(feats_all, s, e)[...] for e in range(2)], axis=0)
        for m in range(0, rows, M_CHUNK):
            at = pl.ds(m, M_CHUNK)
            acc_one[at, :] += _dot(adj_ring[slot, at, :], right)
        fetch(s + SLOTS)
        return carry

    lax.fori_loop(0, 16, step_one, 0)

    aggs_all[me] = acc_one[...].astype(BF16)
    send_own(1, aggs_all)

    def step_two(s, carry):
        gather_step(1, aggs_all, s)
        for e in range(2):
            pre = _dot(piece(aggs_all, s, e)[...], w_one_b[...])
            hid[pl.ds(e * quarter, quarter), :] = jnp.maximum(pre, 0.0).astype(BF16)
        n = s + 16
        for e in range(2):
            slab_copy(n, e).wait()
        slot = lax.rem(n, SLOTS)
        right = hid[...]
        for m in range(0, rows, M_CHUNK):
            at = pl.ds(m, M_CHUNK)
            acc_two[at, :] += _dot(adj_ring[slot, at, :], right)
        fetch(n + SLOTS)
        return carry

    lax.fori_loop(0, 16, step_two, 0)

    count_move(2).wait_recv()
    total = (count[2] + count_in[2])[0:1, 0:1]
    agg_two[...] = acc_two[...].astype(BF16)
    logits = _dot_nt(w_two_t[0:48, :], agg_two[...])[:classes, :]
    weight = mask_v[...].astype(F32)
    shifted = logits - jnp.max(logits, axis=0, keepdims=True)
    log_prob = shifted - jnp.log(jnp.sum(jnp.exp(shifted), axis=0, keepdims=True))
    onehot = (lax.broadcasted_iota(jnp.int32, (classes, rows), 0) == lab_v[...]).astype(F32)
    picked = jnp.sum(onehot * log_prob, axis=0, keepdims=True)
    loss_sum = -jnp.sum(weight * picked)
    grad_t[:classes, :] = (weight * (jnp.exp(log_prob) - onehot) / total).astype(BF16)
    back_t[...] = _dot(w_two_b[...], grad_t[...]).astype(BF16)

    def pair_move(u):
        return remote(stage.at[lax.rem(u, 4)], from_pair.at[u], pair_send.at[lax.rem(u, 4)], pair_recv.at[u], pair)

    def chip_move(u):
        link = lax.rem(u, 2)
        dev = me + (1 - link) * to_x + link * to_y
        return remote(own_sums.at[u], from_chip.at[link, u // 2], chip_send.at[u], chip_recv.at[link, u // 2], dev)

    def finish(u):
        pair_move(u).wait_recv()
        own_sums[u] += from_pair[u]

        @pl.when(u < 8)
        def _():
            chip_move(u).start()

    def step_three(u, carry):
        n = u + 32
        slot = lax.rem(n, SLOTS)

        @pl.when(u >= 4)
        def _():
            pair_move(u).wait_send()

        part_copy(n, 0).wait()
        stage[lax.rem(u, 4)] = _dot(back_t[...], adj_ring[slot, :, pl.ds(0, quarter)])
        pair_move(u).start()
        part_copy(n, 1).wait()
        own_sums[u] = _dot(back_t[...], adj_ring[slot, :, pl.ds(quarter, quarter)])
        fetch(n + SLOTS)

        @pl.when(u >= 1)
        def _():
            finish(u - 1)

        return carry

    lax.fori_loop(0, 16, step_three, 0)
    finish(jnp.int32(15))
    for u in range(12, 16):
        pair_move(u).wait_send()

    part_two = _dot(grad_t[0:48, :], agg_two[...])
    small[0, 0:40, :] = part_two[0:classes, 0:128]
    small[0, 40:80, :] = part_two[0:classes, 128:256]
    small[0, 80:96, :] = jnp.full((16, 128), loss_sum, F32)

    def small_move(i):
        return remote(small.at[i], small_in.at[i], small_send.at[i], small_recv.at[i], (pair, x_next, y_next)[i])

    small_move(0).start()
    pre_t[...] = _dot_nt(w_one_t[...], aggs_all[me])

    small_move(0).wait_recv()
    small[1] = small[0] + small_in[0]
    small_move(1).start()

    for k in range(2):
        for link in range(2):
            u = 8 + 2 * k + (1 - link)
            chip_move(2 * k + link).wait_recv()
            own_sums[u] += from_chip[link, k]
            chip_move(u).start()

    for k in range(2):
        for link in range(2):
            j = 2 * link + k
            chip_move(4 + 2 * k + link).wait_recv()
            own_sums[12 + j] += from_chip[link, 2 + k]
    small_move(1).wait_recv()
    small[2] = small[1] + small_in[1]
    small_move(2).start()
    red_one = jnp.zeros((256, 128), F32)
    for k in range(2):
        for link in range(2):
            j = 2 * (1 - link) + k
            chip_move(8 + 2 * k + link).wait_recv()
            d_hidden = own_sums[12 + j] + from_chip[link, 4 + k]
            keep = pre_t[:, pl.ds(j * quarter, quarter)] > 0.0
            grad_one = jnp.where(keep, d_hidden, 0.0).astype(BF16)
            red_one += _dot(grad_one, aggs_all[me, pl.ds(j * quarter, quarter), :])
    red[...] = red_one

    n_half = red.shape[0] // 2
    n_part = n_half // 2
    mine = pl.multiple_of(core * n_half, 8)
    other = pl.multiple_of((1 - core) * n_half, 8)

    move = remote(red.at[pl.ds(other, n_half)], red_pair, red_send.at[0], red_recv.at[0], pair)
    move.start()
    move.wait_recv()
    red_link[...] = red[pl.ds(mine, n_half), :] + red_pair[...]
    moves = [
        remote(red_link.at[pl.ds(i * n_part, n_part)], red_next.at[pl.ds(i * n_part, n_part)],
               red_send.at[1 + i], red_recv.at[1 + i], (x_next, y_next)[i])
        for i in range(2)
    ]
    for m in moves:
        m.start()
    for m in moves:
        m.wait_recv()
    red_pair2 = red_link[...] + red_next[...]
    red_last[0] = red_pair2
    lasts = [
        remote(red_last.at[0, pl.ds(i * n_part, n_part)], red_last.at[1, pl.ds(i * n_part, n_part)],
               red_send.at[3 + i], red_recv.at[3 + i], (y_next, x_next)[i])
        for i in range(2)
    ]
    for m in lasts:
        m.start()
    for m in lasts:
        m.wait_recv()
    red_out[pl.ds(mine, n_half), :] = red_last[0] + red_last[1]
    ref = red_out.at[pl.ds(mine, n_half)]
    back = remote(ref, ref, red_send.at[5], red_recv.at[5], pair)
    back.start()
    ref_in = red_out.at[pl.ds(other, n_half)]
    remote(ref_in, ref_in, red_send.at[5], red_recv.at[5], pair).wait_recv()

    small_move(2).wait_recv()
    summed = small[2] + small_in[2]
    out[0:256, :] = red_out[...]
    out[256:336, :] = summed[0:80, :]
    out[336:352, :] = summed[80:96, :] / total

    move.wait_send()
    for m in moves + lasts + [back]:
        m.wait_send()
    for i in range(3):
        count_move(i).wait_send()
        small_move(i).wait_send()
    for ph, buf in ((0, feats_all), (1, aggs_all)):
        for to in range(2, 16):
            for e in range(2):
                send_piece(ph, buf, to, e, to, pair).wait_send()
    for u in range(12):
        chip_move(u).wait_send()


def _finish(sums, out_loss, out_one, out_two):
    classes = out_two.shape[0]
    out_one[...] = sums[0:256, :].T
    out_two[:, 0:128] = sums[256:256 + classes, :]
    out_two[:, 128:256] = sums[256 + classes:256 + 2 * classes, :]
    out_loss[...] = sums[336:337, 0:1]


def solution(mesh):
    def step(adj, feat, w_one, w_two, labels, mask):
        rows, nodes = adj.shape
        feat_dim, hidden = w_one.shape
        classes = w_two.shape[1]
        parts = nodes // rows
        any_spec = pl.BlockSpec(memory_space=pltpu.HBM)
        vmem = pl.BlockSpec(memory_space=pltpu.VMEM)
        quarter = rows // 4
        scratch = [
            pltpu.VMEM((parts, rows, feat_dim), BF16),
            pltpu.VMEM((parts, rows, feat_dim), BF16),
            pltpu.VMEM((rows // 2, hidden), BF16),
            pltpu.VMEM((rows, feat_dim), F32),
            pltpu.VMEM((rows, hidden), F32),
            pltpu.VMEM((rows, hidden), BF16),
            pltpu.VMEM((hidden, rows), BF16),
            pltpu.VMEM((128, rows), BF16),
            pltpu.VMEM((hidden, rows), F32),
            pltpu.VMEM((16, hidden, quarter), F32),
            pltpu.VMEM((4, hidden, quarter), F32),
            pltpu.VMEM((16, hidden, quarter), F32),
            pltpu.VMEM((2, 6, hidden, quarter), F32),
            pltpu.VMEM((SLOTS, rows, rows // 2), BF16),
            pltpu.VMEM((feat_dim, hidden), F32),
            pltpu.VMEM((classes, hidden), F32),
            pltpu.VMEM((feat_dim, hidden), BF16),
            pltpu.VMEM((hidden, feat_dim), BF16),
            pltpu.VMEM((hidden, 128), BF16),
            pltpu.VMEM((128, hidden), BF16),
            pltpu.VMEM((1, rows), jnp.int32),
            pltpu.VMEM((1, rows), jnp.int32),
            pltpu.VMEM((3, 8, 128), F32),
            pltpu.VMEM((3, 8, 128), F32),
            pltpu.VMEM((256, 128), F32),
            pltpu.VMEM((128, 128), F32),
            pltpu.VMEM((128, 128), F32),
            pltpu.VMEM((128, 128), F32),
            pltpu.VMEM((2, 128, 128), F32),
            pltpu.VMEM((256, 128), F32),
            pltpu.VMEM((3, 96, 128), F32),
            pltpu.VMEM((3, 96, 128), F32),
            pltpu.SemaphoreType.DMA((SLOTS, 2)),
            pltpu.SemaphoreType.DMA((5,)),
            pltpu.SemaphoreType.DMA((2, 32)),
            pltpu.SemaphoreType.DMA((2, 32)),
            pltpu.SemaphoreType.DMA((3,)),
            pltpu.SemaphoreType.DMA((3,)),
            pltpu.SemaphoreType.DMA((4,)),
            pltpu.SemaphoreType.DMA((16,)),
            pltpu.SemaphoreType.DMA((12,)),
            pltpu.SemaphoreType.DMA((2, 6)),
            pltpu.SemaphoreType.DMA((6,)),
            pltpu.SemaphoreType.DMA((6,)),
            pltpu.SemaphoreType.DMA((3,)),
            pltpu.SemaphoreType.DMA((3,)),
        ]
        sums = pl.pallas_call(
            _kernel,
            out_shape=jax.ShapeDtypeStruct((352, 128), F32),
            in_specs=[any_spec] * 6,
            out_specs=vmem,
            scratch_shapes=scratch,
            compiler_params=pltpu.CompilerParams(
                collective_id=0, has_side_effects=True, vmem_limit_bytes=67_000_000),
            name="gcn_step",
        )(adj, feat, w_one, w_two.T, labels.reshape(1, rows), mask.reshape(1, rows))
        loss, dw_one, dw_two_t = pl.pallas_call(
            _finish,
            out_shape=(
                jax.ShapeDtypeStruct((1, 1), F32),
                jax.ShapeDtypeStruct((feat_dim, hidden), F32),
                jax.ShapeDtypeStruct((classes, hidden), F32),
            ),
            in_specs=[vmem],
            out_specs=(vmem, vmem, vmem),
            name="gcn_finish",
        )(sums)
        return loss.reshape(1), dw_one, dw_two_t.T

    return jax.shard_map(
        step,
        mesh=mesh,
        in_specs=(P(AXIS, None), P(AXIS, None), P(None, None), P(None, None), P(AXIS), P(AXIS)),
        out_specs=(P(None), P(None, None), P(None, None)),
        check_vma=False,
    )
```

```python
import jax
import jax.numpy as jnp
from jax import lax
from jax.experimental import pallas as pl
from jax.experimental.pallas import tpu as pltpu
from jax.sharding import PartitionSpec as P

AXIS = "nodes"
MESH = pl.DeviceIdType.MESH
F32 = jnp.float32
BF16 = jnp.bfloat16

SLOTS = 3
M_CHUNK = 512


def _dot(a, b):
    return jnp.dot(a, b, preferred_element_type=F32)


def _dot_nt(a, b):
    return lax.dot_general(a, b, (((1,), (1,)), ((), ())), preferred_element_type=F32)


def _kernel(
    adj, feat, w_one, w_two, labels, mask,
    out,
    feats_all, aggs_all, hid, acc_one, acc_two, agg_two, back_t, grad_t, pre_t,
    own_part, own_sums, stage, from_pair, to_chip, from_chip, adj_buf,
    w_one_f, w_two_f, w_one_b, w_one_t, w_two_b, w_two_t, lab_v, mask_v, count, count_in,
    red, red_pair, red_link, red_next, red_last, red_out, small, small_in,
    adj_sem, load_sem, gather_send, gather_recv, count_send, count_recv,
    pair_send, pair_recv, pair_free, chip_send, chip_recv, red_send, red_recv, small_send, small_recv, relay_send,
):
    rows = feat.shape[0]
    quarter = rows // 4
    classes = w_two.shape[0]
    me = lax.axis_index(AXIS)
    core, chip_x, chip_y = lax.rem(me, 2), lax.rem(me // 2, 2), me // 4
    to_pair, to_x, to_y = 1 - 2 * core, 2 - 4 * chip_x, 4 - 8 * chip_y
    pair, x_next, y_next = me + to_pair, me + to_x, me + to_y

    def remote(src, dst, send, recv, dev):
        return pltpu.make_async_remote_copy(
            src_ref=src, dst_ref=dst, send_sem=send, recv_sem=recv, device_id=(dev,), device_id_type=MESH)

    def gather_place(s, e):
        low = 1 - (s + 12) // 16
        far = s // 12
        near = 1 - low - far
        flip = low * (s // 2) + (1 - low) * lax.rem(s, 2)
        blk = me + flip * to_pair + (near * (1 - e) + far) * to_x + (near * e + far) * to_y
        part = (low * (2 * lax.rem(s, 2) + e) + near * lax.rem(s // 2 + 2 + 2 * e, 4) + far * (s // 2 - 6 + 2 * e))
        return blk, part

    def reduce_place(u):
        own = u // 12
        diag = 1 - (u + 12) // 16
        near = 1 - own - diag
        link = lax.rem(u, 2)
        nx = diag + near * (1 - link)
        ny = diag + near * link
        part = own * (u - 12) + diag * (2 * link + u // 2) + near * (u // 2 - 2)
        return me + nx * to_x + ny * to_y, part

    def adj_copy(place, slot, e):
        blk, part = place
        col = pl.multiple_of(blk * rows + part * quarter, quarter)
        return pltpu.make_async_copy(
            adj.at[:, pl.ds(col, quarter)], adj_buf.at[slot, :, pl.ds(e * quarter, quarter)], adj_sem.at[slot, e])

    def kept_copy(s, e):
        return adj_copy(gather_place(s, e), SLOTS + s, e)

    def slab_copy(r, e):
        return adj_copy(gather_place(lax.rem(r, 12) + 4, e), lax.rem(r, SLOTS), e)

    def part_copy(r, e):
        blk, part = reduce_place(r - 24)
        return adj_copy((blk + to_pair * (1 - e), part), lax.rem(r, SLOTS), e)

    def fetch(r):
        @pl.when((r >= SLOTS) & (r < 24))
        def _():
            for e in range(2):
                slab_copy(r, e).start()

        @pl.when((r >= 24) & (r < 36))
        def _():
            for e in range(2):
                part_copy(r, e).start()

    loads = [
        pltpu.make_async_copy(feat, feats_all.at[me], load_sem.at[0]),
        pltpu.make_async_copy(mask, mask_v, load_sem.at[1]),
        pltpu.make_async_copy(w_one, w_one_f, load_sem.at[2]),
        pltpu.make_async_copy(w_two, w_two_f, load_sem.at[3]),
        pltpu.make_async_copy(labels, lab_v, load_sem.at[4]),
    ]
    for load in loads:
        load.start()
    for n in range(4):
        for e in range(2):
            kept_copy(n, e).start()
    for n in range(SLOTS):
        for e in range(2):
            slab_copy(n, e).start()

    barrier = pltpu.get_barrier_semaphore()
    for dev in (pair, x_next, y_next):
        pl.semaphore_signal(barrier, inc=1, device_id=(dev,), device_id_type=MESH)
    acc_one[...] = jnp.zeros_like(acc_one)
    acc_two[...] = jnp.zeros_like(acc_two)
    grad_t[...] = jnp.zeros_like(grad_t)
    pl.semaphore_wait(barrier, 3)

    def piece(buf, s, e):
        blk, part = gather_place(s, e)
        return buf.at[blk, pl.ds(pl.multiple_of(part * quarter, quarter), quarter), :]

    def send_piece(ph, buf, s, e, to, dev):
        ref = piece(buf, s, e)
        at = 2 * to + e
        return remote(ref, ref, gather_send.at[ph, at], gather_recv.at[ph, at], dev)

    def send_own(ph, buf):
        for i in range(4):
            for e, dev in ((0, x_next), (1, y_next)):
                part = (i + 2 * e) % 4
                ref = buf.at[me, pl.ds(part * quarter, quarter), :]
                at = 2 * (4 + 2 * i) + e
                remote(ref, ref, gather_send.at[ph, at], gather_recv.at[ph, at], dev).start()

    def gather_step(ph, buf, s):
        for e in range(2):
            @pl.when(s >= 2)
            def _():
                send_piece(ph, buf, s, e, s, pair).wait_recv()

            @pl.when((s == 4) | (s == 6))
            def _():
                send_piece(ph, buf, s, e, s + 8, (y_next, x_next)[e]).start()

            @pl.when(s < 2)
            def _():
                send_piece(ph, buf, s, e, s + 2, pair).start()

            @pl.when((s >= 4) & (lax.rem(s, 2) == 0))
            def _():
                send_piece(ph, buf, s, e, s + 1, pair).start()

    def count_move(i):
        return remote(count.at[i], count_in.at[i], count_send.at[i], count_recv.at[i], (pair, x_next, y_next)[i])

    loads[0].wait()
    send_own(0, feats_all)
    for load in loads[1:]:
        load.wait()
    count[0] = jnp.full((8, 128), jnp.sum(mask_v[...].astype(F32)), F32)
    count_move(0).start()
    w_one_b[...] = w_one_f[...].astype(BF16)
    w_one_t[...] = w_one_f[...].T.astype(BF16)
    w_two_t[...] = jnp.zeros_like(w_two_t)
    w_two_t[:classes, :] = w_two_f[...].astype(BF16)
    w_two_b[...] = w_two_t[...].astype(F32).T.astype(BF16)

    def step_one(s, carry):
        gather_step(0, feats_all, s)

        for i, when in enumerate((1, 12)):
            @pl.when(s == when)
            def _(i=i):
                count_move(i).wait_recv()
                count[i + 1] = count[i] + count_in[i]
                count_move(i + 1).start()

        kept = 1 - (s + 12) // 16
        slot = kept * (SLOTS + s) + (1 - kept) * lax.rem(s + 8, SLOTS)
        for e in range(2):
            adj_copy(gather_place(s, e), slot, e).wait()
        right = jnp.concatenate([piece(feats_all, s, e)[...] for e in range(2)], axis=0)
        for m in range(0, rows, M_CHUNK):
            at = pl.ds(m, M_CHUNK)
            acc_one[at, :] += _dot(adj_buf[slot, at, :], right)
        fetch(s - 4 + SLOTS)
        return carry

    lax.fori_loop(0, 16, step_one, 0)

    aggs_all[me] = acc_one[...].astype(BF16)
    send_own(1, aggs_all)

    def hidden_step(s):
        for e in range(2):
            pre = _dot(piece(aggs_all, s, e)[...], w_one_b[...])
            hid[lax.rem(s, 2), pl.ds(e * quarter, quarter), :] = jnp.maximum(pre, 0.0).astype(BF16)

    def step_two(s, carry):
        @pl.when(s < 15)
        def _():
            gather_step(1, aggs_all, s + 1)

        kept = 1 - (s + 12) // 16
        slot = kept * (SLOTS + s) + (1 - kept) * lax.rem(s + 8, SLOTS)

        @pl.when(s >= 4)
        def _():
            for e in range(2):
                adj_copy(gather_place(s, e), slot, e).wait()

        hidden_step(jnp.minimum(s + 1, 15))
        right = hid[lax.rem(s, 2)]
        for m in range(0, rows, M_CHUNK):
            at = pl.ds(m, M_CHUNK)
            acc_two[at, :] += _dot(adj_buf[slot, at, :], right)

        @pl.when(s >= 4)
        def _():
            fetch(s + 8 + SLOTS)

        return carry

    gather_step(1, aggs_all, jnp.int32(0))
    hidden_step(jnp.int32(0))
    lax.fori_loop(0, 16, step_two, 0)

    count_move(2).wait_recv()
    total = (count[2] + count_in[2])[0:1, 0:1]
    agg_two[...] = acc_two[...].astype(BF16)
    logits = _dot_nt(w_two_t[0:48, :], agg_two[...])[:classes, :]
    weight = mask_v[...].astype(F32)
    shifted = logits - jnp.max(logits, axis=0, keepdims=True)
    log_prob = shifted - jnp.log(jnp.sum(jnp.exp(shifted), axis=0, keepdims=True))
    onehot = (lax.broadcasted_iota(jnp.int32, (classes, rows), 0) == lab_v[...]).astype(F32)
    picked = jnp.sum(onehot * log_prob, axis=0, keepdims=True)
    loss_sum = -jnp.sum(weight * picked)
    grad_t[:classes, :] = (weight * (jnp.exp(log_prob) - onehot) / total).astype(BF16)
    back_t[...] = _dot(w_two_b[...], grad_t[...]).astype(BF16)

    def pair_move(u):
        at = lax.rem(u, 4)
        return remote(stage.at[at], from_pair.at[at], pair_send.at[at], pair_recv.at[u], pair)

    def chip_move(u):
        link = lax.rem(u, 2)
        dev = me + (1 - link) * to_x + link * to_y
        return remote(to_chip.at[u], from_chip.at[link, u // 2], chip_send.at[u], chip_recv.at[link, u // 2], dev)

    def finish(u):
        pair_move(u).wait_recv()
        both = own_part[lax.rem(u, 2)] + from_pair[lax.rem(u, 4)]

        @pl.when(u < 12)
        def _():
            to_chip[u] = both.astype(BF16)
            chip_move(u).start()
            pl.semaphore_signal(pair_free, inc=1, device_id=(pair,), device_id_type=MESH)

        @pl.when(u >= 12)
        def _():
            own_sums[u - 12] = both

    def step_three(u, carry):
        r = u + 24
        ring = 1 - u // 12
        kept = (1 - ring) * (u - 12)
        slots = [ring * lax.rem(r, SLOTS) + (1 - ring) * (SLOTS + 2 * (1 - e) + kept // 2) for e in range(2)]
        cols = [pl.multiple_of((ring * e + lax.rem(kept, 2)) * quarter, quarter) for e in range(2)]

        @pl.when(u >= 4)
        def _():
            pair_move(u).wait_send()
            pl.semaphore_wait(pair_free, 1)

        @pl.when(u < 12)
        def _():
            part_copy(r, 0).wait()

        stage[lax.rem(u, 4)] = _dot(back_t[...], adj_buf[slots[0], :, pl.ds(cols[0], quarter)])
        pair_move(u).start()

        @pl.when(u < 12)
        def _():
            part_copy(r, 1).wait()

        own_part[lax.rem(u, 2)] = _dot(back_t[...], adj_buf[slots[1], :, pl.ds(cols[1], quarter)])
        fetch(r + SLOTS)

        @pl.when(u >= 1)
        def _():
            finish(u - 1)

        return carry

    lax.fori_loop(0, 16, step_three, 0)
    finish(jnp.int32(15))
    for u in range(12, 16):
        pair_move(u).wait_send()

    part_two = _dot(grad_t[0:48, :], agg_two[...])
    small[0, 0:40, :] = part_two[0:classes, 0:128]
    small[0, 40:80, :] = part_two[0:classes, 128:256]
    small[0, 80:96, :] = jnp.full((16, 128), loss_sum, F32)

    def small_move(i):
        return remote(small.at[i], small_in.at[i], small_send.at[i], small_recv.at[i], (pair, x_next, y_next)[i])

    small_move(0).start()
    pre_t[...] = _dot_nt(w_one_t[...], aggs_all[me])

    small_move(0).wait_recv()
    small[1] = small[0] + small_in[0]
    small_move(1).start()

    relays = []
    for k in range(2):
        for link in range(2):
            chip_move(2 * k + link).wait_recv()
            move = remote(from_chip.at[link, k], from_chip.at[1 - link, 6 + k], relay_send.at[link, k],
                          chip_recv.at[1 - link, 6 + k], (y_next, x_next)[link])
            move.start()
            relays.append(move)

    for j in range(4):
        for link in range(2):
            chip_move(4 + 2 * j + link).wait_recv()
            own_sums[j] += from_chip[link, 2 + j].astype(F32)
    small_move(1).wait_recv()
    small[2] = small[1] + small_in[1]
    small_move(2).start()
    red_one = jnp.zeros((256, 128), F32)
    for k in range(2):
        for link in range(2):
            j = 2 * (1 - link) + k
            relays[2 * k + 1 - link].wait_recv()
            d_hidden = own_sums[j] + from_chip[link, 6 + k].astype(F32)
            keep = pre_t[:, pl.ds(j * quarter, quarter)] > 0.0
            grad_one = jnp.where(keep, d_hidden, 0.0).astype(BF16)
            red_one += _dot(grad_one, aggs_all[me, pl.ds(j * quarter, quarter), :])
    red[...] = red_one

    n_half = red.shape[0] // 2
    n_part = n_half // 2
    mine = pl.multiple_of(core * n_half, 8)
    other = pl.multiple_of((1 - core) * n_half, 8)

    move = remote(red.at[pl.ds(other, n_half)], red_pair, red_send.at[0], red_recv.at[0], pair)
    move.start()
    move.wait_recv()
    red_link[...] = red[pl.ds(mine, n_half), :] + red_pair[...]
    moves = [
        remote(red_link.at[pl.ds(i * n_part, n_part)], red_next.at[pl.ds(i * n_part, n_part)],
               red_send.at[1 + i], red_recv.at[1 + i], (x_next, y_next)[i])
        for i in range(2)
    ]
    for m in moves:
        m.start()
    for m in moves:
        m.wait_recv()
    red_pair2 = red_link[...] + red_next[...]
    red_last[0] = red_pair2
    lasts = [
        remote(red_last.at[0, pl.ds(i * n_part, n_part)], red_last.at[1, pl.ds(i * n_part, n_part)],
               red_send.at[3 + i], red_recv.at[3 + i], (y_next, x_next)[i])
        for i in range(2)
    ]
    for m in lasts:
        m.start()
    for m in lasts:
        m.wait_recv()
    red_out[pl.ds(mine, n_half), :] = red_last[0] + red_last[1]
    ref = red_out.at[pl.ds(mine, n_half)]
    back = remote(ref, ref, red_send.at[5], red_recv.at[5], pair)
    back.start()
    ref_in = red_out.at[pl.ds(other, n_half)]
    remote(ref_in, ref_in, red_send.at[5], red_recv.at[5], pair).wait_recv()

    small_move(2).wait_recv()
    summed = small[2] + small_in[2]
    out[0:256, :] = red_out[...]
    out[256:336, :] = summed[0:80, :]
    out[336:352, :] = summed[80:96, :] / total

    move.wait_send()
    for m in moves + lasts + [back]:
        m.wait_send()
    for i in range(3):
        count_move(i).wait_send()
        small_move(i).wait_send()
    for ph, buf in ((0, feats_all), (1, aggs_all)):
        for to in range(2, 16):
            for e in range(2):
                send_piece(ph, buf, to, e, to, pair).wait_send()
    for u in range(12):
        chip_move(u).wait_send()
    for relay in relays:
        relay.wait_send()


def _finish(sums, out_loss, out_one, out_two):
    classes = out_two.shape[0]
    out_one[...] = sums[0:256, :].T
    out_two[:, 0:128] = sums[256:256 + classes, :]
    out_two[:, 128:256] = sums[256 + classes:256 + 2 * classes, :]
    out_loss[...] = sums[336:337, 0:1]


def solution(mesh):
    def step(adj, feat, w_one, w_two, labels, mask):
        rows, nodes = adj.shape
        feat_dim, hidden = w_one.shape
        classes = w_two.shape[1]
        parts = nodes // rows
        any_spec = pl.BlockSpec(memory_space=pltpu.HBM)
        vmem = pl.BlockSpec(memory_space=pltpu.VMEM)
        quarter = rows // 4
        scratch = [
            pltpu.VMEM((parts, rows, feat_dim), BF16),
            pltpu.VMEM((parts, rows, feat_dim), BF16),
            pltpu.VMEM((2, rows // 2, hidden), BF16),
            pltpu.VMEM((rows, feat_dim), F32),
            pltpu.VMEM((rows, hidden), F32),
            pltpu.VMEM((rows, hidden), BF16),
            pltpu.VMEM((hidden, rows), BF16),
            pltpu.VMEM((128, rows), BF16),
            pltpu.VMEM((hidden, rows), F32),
            pltpu.VMEM((2, hidden, quarter), F32),
            pltpu.VMEM((4, hidden, quarter), F32),
            pltpu.VMEM((4, hidden, quarter), F32),
            pltpu.VMEM((4, hidden, quarter), F32),
            pltpu.VMEM((12, hidden, quarter), BF16),
            pltpu.VMEM((2, 8, hidden, quarter), BF16),
            pltpu.VMEM((SLOTS + 4, rows, rows // 2), BF16),
            pltpu.VMEM((feat_dim, hidden), F32),
            pltpu.VMEM((classes, hidden), F32),
            pltpu.VMEM((feat_dim, hidden), BF16),
            pltpu.VMEM((hidden, feat_dim), BF16),
            pltpu.VMEM((hidden, 128), BF16),
            pltpu.VMEM((128, hidden), BF16),
            pltpu.VMEM((1, rows), jnp.int32),
            pltpu.VMEM((1, rows), jnp.int32),
            pltpu.VMEM((3, 8, 128), F32),
            pltpu.VMEM((3, 8, 128), F32),
            pltpu.VMEM((256, 128), F32),
            pltpu.VMEM((128, 128), F32),
            pltpu.VMEM((128, 128), F32),
            pltpu.VMEM((128, 128), F32),
            pltpu.VMEM((2, 128, 128), F32),
            pltpu.VMEM((256, 128), F32),
            pltpu.VMEM((3, 96, 128), F32),
            pltpu.VMEM((3, 96, 128), F32),
            pltpu.SemaphoreType.DMA((SLOTS + 4, 2)),
            pltpu.SemaphoreType.DMA((5,)),
            pltpu.SemaphoreType.DMA((2, 32)),
            pltpu.SemaphoreType.DMA((2, 32)),
            pltpu.SemaphoreType.DMA((3,)),
            pltpu.SemaphoreType.DMA((3,)),
            pltpu.SemaphoreType.DMA((4,)),
            pltpu.SemaphoreType.DMA((16,)),
            pltpu.SemaphoreType.REGULAR,
            pltpu.SemaphoreType.DMA((12,)),
            pltpu.SemaphoreType.DMA((2, 8)),
            pltpu.SemaphoreType.DMA((6,)),
            pltpu.SemaphoreType.DMA((6,)),
            pltpu.SemaphoreType.DMA((3,)),
            pltpu.SemaphoreType.DMA((3,)),
            pltpu.SemaphoreType.DMA((2, 2)),
        ]
        sums = pl.pallas_call(
            _kernel,
            out_shape=jax.ShapeDtypeStruct((352, 128), F32),
            in_specs=[any_spec] * 6,
            out_specs=vmem,
            scratch_shapes=scratch,
            compiler_params=pltpu.CompilerParams(
                collective_id=0, has_side_effects=True, vmem_limit_bytes=67_000_000),
            name="gcn_step",
        )(adj, feat, w_one, w_two.T, labels.reshape(1, rows), mask.reshape(1, rows))
        loss, dw_one, dw_two_t = pl.pallas_call(
            _finish,
            out_shape=(
                jax.ShapeDtypeStruct((1, 1), F32),
                jax.ShapeDtypeStruct((feat_dim, hidden), F32),
                jax.ShapeDtypeStruct((classes, hidden), F32),
            ),
            in_specs=[vmem],
            out_specs=(vmem, vmem, vmem),
            name="gcn_finish",
        )(sums)
        return loss.reshape(1), dw_one, dw_two_t.T

    return jax.shard_map(
        step,
        mesh=mesh,
        in_specs=(P(AXIS, None), P(AXIS, None), P(None, None), P(None, None), P(AXIS), P(AXIS)),
        out_specs=(P(None), P(None, None), P(None, None)),
        check_vma=False,
    )
```

```python
import jax
import jax.numpy as jnp
from jax import lax
from jax.experimental import pallas as pl
from jax.experimental.pallas import tpu as pltpu
from jax.sharding import PartitionSpec as P

AXIS = "nodes"
MESH = pl.DeviceIdType.MESH
F32 = jnp.float32
BF16 = jnp.bfloat16

SLOTS = 3
M_CHUNK = 512


def _dot(a, b):
    return jnp.dot(a, b, preferred_element_type=F32)


def _dot_nt(a, b):
    return lax.dot_general(a, b, (((1,), (1,)), ((), ())), preferred_element_type=F32)


def _kernel(
    adj, feat, w_one, w_two, labels, mask,
    out,
    feats_all, aggs_all, hid, acc_one, acc_two, agg_two, back_t, grad_t, pre_t,
    own_part, own_sums, stage, from_pair, to_chip, from_chip, adj_buf,
    w_one_f, w_two_f, w_one_b, w_one_t, w_two_b, w_two_t, lab_v, mask_v, count, count_in,
    red, red_pair, red_link, red_next, red_last, red_out, small, small_in,
    adj_sem, load_sem, gather_send, gather_recv, count_send, count_recv,
    pair_send, pair_recv, pair_free, chip_send, chip_recv, red_send, red_recv, small_send, small_recv, relay_send,
):
    rows = feat.shape[0]
    quarter = rows // 4
    classes = w_two.shape[0]
    me = lax.axis_index(AXIS)
    core, chip_x, chip_y = lax.rem(me, 2), lax.rem(me // 2, 2), me // 4
    to_pair, to_x, to_y = 1 - 2 * core, 2 - 4 * chip_x, 4 - 8 * chip_y
    pair, x_next, y_next = me + to_pair, me + to_x, me + to_y

    def remote(src, dst, send, recv, dev):
        return pltpu.make_async_remote_copy(
            src_ref=src, dst_ref=dst, send_sem=send, recv_sem=recv, device_id=(dev,), device_id_type=MESH)

    def gather_place(s, e):
        low = 1 - (s + 12) // 16
        far = s // 12
        near = 1 - low - far
        flip = low * (s // 2) + (1 - low) * lax.rem(s, 2)
        blk = me + flip * to_pair + (near * (1 - e) + far) * to_x + (near * e + far) * to_y
        part = (low * (2 * lax.rem(s, 2) + e) + near * lax.rem(s // 2 + 2 + 2 * e, 4) + far * (s // 2 - 6 + 2 * e))
        return blk, part

    def reduce_place(u):
        own = u // 12
        diag = 1 - (u + 12) // 16
        near = 1 - own - diag
        link = lax.rem(u, 2)
        nx = diag + near * (1 - link)
        ny = diag + near * link
        part = own * (u - 12) + diag * (2 * link + u // 2) + near * (u // 2 - 2)
        return me + nx * to_x + ny * to_y, part

    def adj_copy(place, slot, e):
        blk, part = place
        col = pl.multiple_of(blk * rows + part * quarter, quarter)
        return pltpu.make_async_copy(
            adj.at[:, pl.ds(col, quarter)], adj_buf.at[slot, :, pl.ds(e * quarter, quarter)], adj_sem.at[slot, e])

    def kept_copy(s, e):
        return adj_copy(gather_place(s, e), SLOTS + s, e)

    def slab_copy(r, e):
        return adj_copy(gather_place(lax.rem(r, 12) + 4, e), lax.rem(r, SLOTS), e)

    def part_copy(r, e):
        blk, part = reduce_place(r - 24)
        return adj_copy((blk + to_pair * (1 - e), part), lax.rem(r, SLOTS), e)

    def fetch(r):
        @pl.when((r >= SLOTS) & (r < 24))
        def _():
            for e in range(2):
                slab_copy(r, e).start()

        @pl.when((r >= 24) & (r < 36))
        def _():
            for e in range(2):
                part_copy(r, e).start()

    loads = [
        pltpu.make_async_copy(feat, feats_all.at[me], load_sem.at[0]),
        pltpu.make_async_copy(mask, mask_v, load_sem.at[1]),
        pltpu.make_async_copy(w_one, w_one_f, load_sem.at[2]),
        pltpu.make_async_copy(w_two, w_two_f, load_sem.at[3]),
        pltpu.make_async_copy(labels, lab_v, load_sem.at[4]),
    ]
    for load in loads:
        load.start()
    for e in range(2):
        kept_copy(0, e).start()

    barrier = pltpu.get_barrier_semaphore()
    for dev in (pair, x_next, y_next):
        pl.semaphore_signal(barrier, inc=1, device_id=(dev,), device_id_type=MESH)
    acc_one[...] = jnp.zeros_like(acc_one)
    acc_two[...] = jnp.zeros_like(acc_two)
    grad_t[...] = jnp.zeros_like(grad_t)
    pl.semaphore_wait(barrier, 3)

    def piece(buf, s, e):
        blk, part = gather_place(s, e)
        return buf.at[blk, pl.ds(pl.multiple_of(part * quarter, quarter), quarter), :]

    def send_piece(ph, buf, s, e, to, dev):
        ref = piece(buf, s, e)
        at = 2 * to + e
        return remote(ref, ref, gather_send.at[ph, at], gather_recv.at[ph, at], dev)

    def send_own(ph, buf):
        for i in range(4):
            for e, dev in ((0, x_next), (1, y_next)):
                part = (i + 2 * e) % 4
                ref = buf.at[me, pl.ds(part * quarter, quarter), :]
                at = 2 * (4 + 2 * i) + e
                remote(ref, ref, gather_send.at[ph, at], gather_recv.at[ph, at], dev).start()

    def gather_step(ph, buf, s):
        for e in range(2):
            @pl.when(s >= 2)
            def _():
                send_piece(ph, buf, s, e, s, pair).wait_recv()

            @pl.when((s == 4) | (s == 6))
            def _():
                send_piece(ph, buf, s, e, s + 8, (y_next, x_next)[e]).start()

            @pl.when(s < 2)
            def _():
                send_piece(ph, buf, s, e, s + 2, pair).start()

            @pl.when((s >= 4) & (lax.rem(s, 2) == 0))
            def _():
                send_piece(ph, buf, s, e, s + 1, pair).start()

    def count_move(i):
        return remote(count.at[i], count_in.at[i], count_send.at[i], count_recv.at[i], (pair, x_next, y_next)[i])

    loads[0].wait()
    send_own(0, feats_all)
    for e in range(2):
        kept_copy(1, e).start()
        kept_copy(2, e).start()
    for load in loads[1:]:
        load.wait()
    count[0] = jnp.full((8, 128), jnp.sum(mask_v[...].astype(F32)), F32)
    count_move(0).start()
    w_one_b[...] = w_one_f[...].astype(BF16)
    w_one_t[...] = w_one_f[...].T.astype(BF16)
    w_two_t[...] = jnp.zeros_like(w_two_t)
    w_two_t[:classes, :] = w_two_f[...].astype(BF16)
    w_two_b[...] = w_two_t[...].astype(F32).T.astype(BF16)

    def step_one(s, carry):
        gather_step(0, feats_all, s)

        for i, when in enumerate((1, 12)):
            @pl.when(s == when)
            def _(i=i):
                count_move(i).wait_recv()
                count[i + 1] = count[i] + count_in[i]
                count_move(i + 1).start()

        kept = 1 - (s + 12) // 16
        slot = kept * (SLOTS + s) + (1 - kept) * lax.rem(s + 8, SLOTS)
        for e in range(2):
            adj_copy(gather_place(s, e), slot, e).wait()
        right = jnp.concatenate([piece(feats_all, s, e)[...] for e in range(2)], axis=0)
        for m in range(0, rows, M_CHUNK):
            at = pl.ds(m, M_CHUNK)
            acc_one[at, :] += _dot(adj_buf[slot, at, :], right)
        fetch(s - 4 + SLOTS)

        @pl.when(s == 0)
        def _():
            for e in range(2):
                kept_copy(3, e).start()

        @pl.when((s >= 1) & (s < 1 + SLOTS))
        def _():
            for e in range(2):
                slab_copy(s - 1, e).start()

        return carry

    lax.fori_loop(0, 16, step_one, 0)

    aggs_all[me] = acc_one[...].astype(BF16)
    send_own(1, aggs_all)

    def hidden_step(s):
        for e in range(2):
            pre = _dot(piece(aggs_all, s, e)[...], w_one_b[...])
            hid[lax.rem(s, 2), pl.ds(e * quarter, quarter), :] = jnp.maximum(pre, 0.0).astype(BF16)

    def step_two(s, carry):
        @pl.when(s < 15)
        def _():
            gather_step(1, aggs_all, s + 1)

        kept = 1 - (s + 12) // 16
        slot = kept * (SLOTS + s) + (1 - kept) * lax.rem(s + 8, SLOTS)

        @pl.when(s >= 4)
        def _():
            for e in range(2):
                adj_copy(gather_place(s, e), slot, e).wait()

        hidden_step(jnp.minimum(s + 1, 15))
        right = hid[lax.rem(s, 2)]
        for m in range(0, rows, M_CHUNK):
            at = pl.ds(m, M_CHUNK)
            acc_two[at, :] += _dot(adj_buf[slot, at, :], right)

        @pl.when(s >= 4)
        def _():
            fetch(s + 8 + SLOTS)

        return carry

    gather_step(1, aggs_all, jnp.int32(0))
    hidden_step(jnp.int32(0))
    lax.fori_loop(0, 16, step_two, 0)

    count_move(2).wait_recv()
    total = (count[2] + count_in[2])[0:1, 0:1]
    agg_two[...] = acc_two[...].astype(BF16)
    logits = _dot_nt(w_two_t[0:48, :], agg_two[...])[:classes, :]
    weight = mask_v[...].astype(F32)
    shifted = logits - jnp.max(logits, axis=0, keepdims=True)
    log_prob = shifted - jnp.log(jnp.sum(jnp.exp(shifted), axis=0, keepdims=True))
    onehot = (lax.broadcasted_iota(jnp.int32, (classes, rows), 0) == lab_v[...]).astype(F32)
    picked = jnp.sum(onehot * log_prob, axis=0, keepdims=True)
    loss_sum = -jnp.sum(weight * picked)
    grad_t[:classes, :] = (weight * (jnp.exp(log_prob) - onehot) / total).astype(BF16)
    back_t[...] = _dot(w_two_b[...], grad_t[...]).astype(BF16)

    def pair_move(u):
        at = lax.rem(u, 4)
        return remote(stage.at[at], from_pair.at[at], pair_send.at[at], pair_recv.at[u], pair)

    def chip_move(u):
        link = lax.rem(u, 2)
        dev = me + (1 - link) * to_x + link * to_y
        return remote(to_chip.at[u], from_chip.at[link, u // 2], chip_send.at[u], chip_recv.at[link, u // 2], dev)

    def finish(u):
        pair_move(u).wait_recv()
        both = own_part[lax.rem(u, 2)] + from_pair[lax.rem(u, 4)]

        @pl.when(u < 12)
        def _():
            to_chip[u] = both.astype(BF16)
            chip_move(u).start()
            pl.semaphore_signal(pair_free, inc=1, device_id=(pair,), device_id_type=MESH)

        @pl.when(u >= 12)
        def _():
            own_sums[u - 12] = both

    def step_three(u, carry):
        r = u + 24
        ring = 1 - u // 12
        kept = (1 - ring) * (u - 12)
        slots = [ring * lax.rem(r, SLOTS) + (1 - ring) * (SLOTS + 2 * (1 - e) + kept // 2) for e in range(2)]
        cols = [pl.multiple_of((ring * e + lax.rem(kept, 2)) * quarter, quarter) for e in range(2)]

        @pl.when(u >= 4)
        def _():
            pair_move(u).wait_send()
            pl.semaphore_wait(pair_free, 1)

        @pl.when(u < 12)
        def _():
            part_copy(r, 0).wait()

        stage[lax.rem(u, 4)] = _dot(back_t[...], adj_buf[slots[0], :, pl.ds(cols[0], quarter)])
        pair_move(u).start()

        @pl.when(u >= 1)
        def _():
            finish(u - 1)

        @pl.when(u < 12)
        def _():
            part_copy(r, 1).wait()

        own_part[lax.rem(u, 2)] = _dot(back_t[...], adj_buf[slots[1], :, pl.ds(cols[1], quarter)])
        fetch(r + SLOTS)
        return carry

    lax.fori_loop(0, 16, step_three, 0)
    finish(jnp.int32(15))
    for u in range(12, 16):
        pair_move(u).wait_send()

    part_two = _dot(grad_t[0:48, :], agg_two[...])
    small[0, 0:40, :] = part_two[0:classes, 0:128]
    small[0, 40:80, :] = part_two[0:classes, 128:256]
    small[0, 80:96, :] = jnp.full((16, 128), loss_sum, F32)

    def small_move(i):
        return remote(small.at[i], small_in.at[i], small_send.at[i], small_recv.at[i], (pair, x_next, y_next)[i])

    small_move(0).start()
    pre_t[...] = _dot_nt(w_one_t[...], aggs_all[me])

    small_move(0).wait_recv()
    small[1] = small[0] + small_in[0]
    small_move(1).start()

    relays = []
    for k in range(2):
        for link in range(2):
            chip_move(2 * k + link).wait_recv()
            move = remote(from_chip.at[link, k], from_chip.at[1 - link, 6 + k], relay_send.at[link, k],
                          chip_recv.at[1 - link, 6 + k], (y_next, x_next)[link])
            move.start()
            relays.append(move)

    for j in range(4):
        for link in range(2):
            chip_move(4 + 2 * j + link).wait_recv()
            own_sums[j] += from_chip[link, 2 + j].astype(F32)
    small_move(1).wait_recv()
    small[2] = small[1] + small_in[1]
    small_move(2).start()
    red_one = jnp.zeros((256, 128), F32)
    for k in range(2):
        for link in range(2):
            j = 2 * (1 - link) + k
            relays[2 * k + 1 - link].wait_recv()
            d_hidden = own_sums[j] + from_chip[link, 6 + k].astype(F32)
            keep = pre_t[:, pl.ds(j * quarter, quarter)] > 0.0
            grad_one = jnp.where(keep, d_hidden, 0.0).astype(BF16)
            red_one += _dot(grad_one, aggs_all[me, pl.ds(j * quarter, quarter), :])
    red[...] = red_one

    n_half = red.shape[0] // 2
    n_part = n_half // 2
    mine = pl.multiple_of(core * n_half, 8)
    other = pl.multiple_of((1 - core) * n_half, 8)

    move = remote(red.at[pl.ds(other, n_half)], red_pair, red_send.at[0], red_recv.at[0], pair)
    move.start()
    move.wait_recv()
    red_link[...] = red[pl.ds(mine, n_half), :] + red_pair[...]
    moves = [
        remote(red_link.at[pl.ds(i * n_part, n_part)], red_next.at[pl.ds(i * n_part, n_part)],
               red_send.at[1 + i], red_recv.at[1 + i], (x_next, y_next)[i])
        for i in range(2)
    ]
    for m in moves:
        m.start()
    for m in moves:
        m.wait_recv()
    red_pair2 = red_link[...] + red_next[...]
    red_last[0] = red_pair2
    lasts = [
        remote(red_last.at[0, pl.ds(i * n_part, n_part)], red_last.at[1, pl.ds(i * n_part, n_part)],
               red_send.at[3 + i], red_recv.at[3 + i], (y_next, x_next)[i])
        for i in range(2)
    ]
    for m in lasts:
        m.start()
    for m in lasts:
        m.wait_recv()
    red_out[pl.ds(mine, n_half), :] = red_last[0] + red_last[1]
    ref = red_out.at[pl.ds(mine, n_half)]
    back = remote(ref, ref, red_send.at[5], red_recv.at[5], pair)
    back.start()
    ref_in = red_out.at[pl.ds(other, n_half)]
    remote(ref_in, ref_in, red_send.at[5], red_recv.at[5], pair).wait_recv()

    small_move(2).wait_recv()
    summed = small[2] + small_in[2]
    out[0:256, :] = red_out[...]
    out[256:336, :] = summed[0:80, :]
    out[336:352, :] = summed[80:96, :] / total

    move.wait_send()
    for m in moves + lasts + [back]:
        m.wait_send()
    for i in range(3):
        count_move(i).wait_send()
        small_move(i).wait_send()
    for ph, buf in ((0, feats_all), (1, aggs_all)):
        for to in range(2, 16):
            for e in range(2):
                send_piece(ph, buf, to, e, to, pair).wait_send()
    for u in range(12):
        chip_move(u).wait_send()
    for relay in relays:
        relay.wait_send()


def _finish(sums, out_loss, out_one, out_two):
    classes = out_two.shape[0]
    out_one[...] = sums[0:256, :].T
    out_two[:, 0:128] = sums[256:256 + classes, :]
    out_two[:, 128:256] = sums[256 + classes:256 + 2 * classes, :]
    out_loss[...] = sums[336:337, 0:1]


def solution(mesh):
    def step(adj, feat, w_one, w_two, labels, mask):
        rows, nodes = adj.shape
        feat_dim, hidden = w_one.shape
        classes = w_two.shape[1]
        parts = nodes // rows
        any_spec = pl.BlockSpec(memory_space=pltpu.HBM)
        vmem = pl.BlockSpec(memory_space=pltpu.VMEM)
        quarter = rows // 4
        scratch = [
            pltpu.VMEM((parts, rows, feat_dim), BF16),
            pltpu.VMEM((parts, rows, feat_dim), BF16),
            pltpu.VMEM((2, rows // 2, hidden), BF16),
            pltpu.VMEM((rows, feat_dim), F32),
            pltpu.VMEM((rows, hidden), F32),
            pltpu.VMEM((rows, hidden), BF16),
            pltpu.VMEM((hidden, rows), BF16),
            pltpu.VMEM((128, rows), BF16),
            pltpu.VMEM((hidden, rows), F32),
            pltpu.VMEM((2, hidden, quarter), F32),
            pltpu.VMEM((4, hidden, quarter), F32),
            pltpu.VMEM((4, hidden, quarter), F32),
            pltpu.VMEM((4, hidden, quarter), F32),
            pltpu.VMEM((12, hidden, quarter), BF16),
            pltpu.VMEM((2, 8, hidden, quarter), BF16),
            pltpu.VMEM((SLOTS + 4, rows, rows // 2), BF16),
            pltpu.VMEM((feat_dim, hidden), F32),
            pltpu.VMEM((classes, hidden), F32),
            pltpu.VMEM((feat_dim, hidden), BF16),
            pltpu.VMEM((hidden, feat_dim), BF16),
            pltpu.VMEM((hidden, 128), BF16),
            pltpu.VMEM((128, hidden), BF16),
            pltpu.VMEM((1, rows), jnp.int32),
            pltpu.VMEM((1, rows), jnp.int32),
            pltpu.VMEM((3, 8, 128), F32),
            pltpu.VMEM((3, 8, 128), F32),
            pltpu.VMEM((256, 128), F32),
            pltpu.VMEM((128, 128), F32),
            pltpu.VMEM((128, 128), F32),
            pltpu.VMEM((128, 128), F32),
            pltpu.VMEM((2, 128, 128), F32),
            pltpu.VMEM((256, 128), F32),
            pltpu.VMEM((3, 96, 128), F32),
            pltpu.VMEM((3, 96, 128), F32),
            pltpu.SemaphoreType.DMA((SLOTS + 4, 2)),
            pltpu.SemaphoreType.DMA((5,)),
            pltpu.SemaphoreType.DMA((2, 32)),
            pltpu.SemaphoreType.DMA((2, 32)),
            pltpu.SemaphoreType.DMA((3,)),
            pltpu.SemaphoreType.DMA((3,)),
            pltpu.SemaphoreType.DMA((4,)),
            pltpu.SemaphoreType.DMA((16,)),
            pltpu.SemaphoreType.REGULAR,
            pltpu.SemaphoreType.DMA((12,)),
            pltpu.SemaphoreType.DMA((2, 8)),
            pltpu.SemaphoreType.DMA((6,)),
            pltpu.SemaphoreType.DMA((6,)),
            pltpu.SemaphoreType.DMA((3,)),
            pltpu.SemaphoreType.DMA((3,)),
            pltpu.SemaphoreType.DMA((2, 2)),
        ]
        sums = pl.pallas_call(
            _kernel,
            out_shape=jax.ShapeDtypeStruct((352, 128), F32),
            in_specs=[any_spec] * 6,
            out_specs=vmem,
            scratch_shapes=scratch,
            compiler_params=pltpu.CompilerParams(
                collective_id=0, has_side_effects=True, vmem_limit_bytes=67_000_000),
            name="gcn_step",
        )(adj, feat, w_one, w_two.T, labels.reshape(1, rows), mask.reshape(1, rows))
        loss, dw_one, dw_two_t = pl.pallas_call(
            _finish,
            out_shape=(
                jax.ShapeDtypeStruct((1, 1), F32),
                jax.ShapeDtypeStruct((feat_dim, hidden), F32),
                jax.ShapeDtypeStruct((classes, hidden), F32),
            ),
            in_specs=[vmem],
            out_specs=(vmem, vmem, vmem),
            name="gcn_finish",
        )(sums)
        return loss.reshape(1), dw_one, dw_two_t.T

    return jax.shard_map(
        step,
        mesh=mesh,
        in_specs=(P(AXIS, None), P(AXIS, None), P(None, None), P(None, None), P(AXIS), P(AXIS)),
        out_specs=(P(None), P(None, None), P(None, None)),
        check_vma=False,
    )
```

```python
import jax
import jax.numpy as jnp
from jax import lax
from jax.experimental import pallas as pl
from jax.experimental.pallas import tpu as pltpu
from jax.sharding import PartitionSpec as P

AXIS = "nodes"
MESH = pl.DeviceIdType.MESH
F32 = jnp.float32
BF16 = jnp.bfloat16

SLOTS = 3
M_CHUNK = 512
M_TWO = 512


def _dot(a, b):
    return jnp.dot(a, b, preferred_element_type=F32)


def _dot_nt(a, b):
    return lax.dot_general(a, b, (((1,), (1,)), ((), ())), preferred_element_type=F32)


def _kernel(
    adj, feat, w_one, w_two, labels, mask,
    out,
    feats_all, aggs_all, hid, hid_next, acc_one, acc_two, agg_two, back_t, grad_t, pre_t,
    own_part, own_sums, stage, from_pair, to_chip, from_chip, adj_buf,
    w_one_f, w_two_f, w_one_b, w_one_t, w_two_b, w_two_t, lab_v, mask_v, count, count_in,
    red, red_pair, red_link, red_next, red_last, red_out, small, small_in,
    adj_sem, load_sem, gather_send, gather_recv, count_send, count_recv,
    pair_send, pair_recv, pair_free, chip_send, chip_recv, red_send, red_recv, small_send, small_recv, relay_send,
):
    rows = feat.shape[0]
    quarter = rows // 4
    classes = w_two.shape[0]
    me = lax.axis_index(AXIS)
    core, chip_x, chip_y = lax.rem(me, 2), lax.rem(me // 2, 2), me // 4
    to_pair, to_x, to_y = 1 - 2 * core, 2 - 4 * chip_x, 4 - 8 * chip_y
    pair, x_next, y_next = me + to_pair, me + to_x, me + to_y

    def remote(src, dst, send, recv, dev):
        return pltpu.make_async_remote_copy(
            src_ref=src, dst_ref=dst, send_sem=send, recv_sem=recv, device_id=(dev,), device_id_type=MESH)

    def gather_place(s, e):
        low = 1 - (s + 12) // 16
        far = s // 12
        near = 1 - low - far
        flip = low * (s // 2) + (1 - low) * lax.rem(s, 2)
        blk = me + flip * to_pair + (near * (1 - e) + far) * to_x + (near * e + far) * to_y
        part = (low * (2 * lax.rem(s, 2) + e) + near * lax.rem(s // 2 + 2 + 2 * e, 4) + far * (s // 2 - 6 + 2 * e))
        return blk, part

    def reduce_place(u):
        own = u // 12
        diag = 1 - (u + 12) // 16
        near = 1 - own - diag
        link = lax.rem(u, 2)
        nx = diag + near * (1 - link)
        ny = diag + near * link
        part = own * (u - 12) + diag * (2 * link + u // 2) + near * (u // 2 - 2)
        return me + nx * to_x + ny * to_y, part

    def adj_copy(place, slot, e):
        blk, part = place
        col = pl.multiple_of(blk * rows + part * quarter, quarter)
        return pltpu.make_async_copy(
            adj.at[:, pl.ds(col, quarter)], adj_buf.at[slot, :, pl.ds(e * quarter, quarter)], adj_sem.at[slot, e])

    def kept_copy(s, e):
        return adj_copy(gather_place(s, e), SLOTS + s, e)

    def slab_copy(r, e):
        return adj_copy(gather_place(lax.rem(r, 12) + 4, e), lax.rem(r, SLOTS), e)

    def part_copy(r, e):
        blk, part = reduce_place(r - 24)
        return adj_copy((blk + to_pair * (1 - e), part), lax.rem(r, SLOTS), e)

    def fetch(r):
        @pl.when((r >= SLOTS) & (r < 24))
        def _():
            for e in range(2):
                slab_copy(r, e).start()

        @pl.when((r >= 24) & (r < 36))
        def _():
            for e in range(2):
                part_copy(r, e).start()

    loads = [
        pltpu.make_async_copy(feat, feats_all.at[me], load_sem.at[0]),
        pltpu.make_async_copy(mask, mask_v, load_sem.at[1]),
        pltpu.make_async_copy(w_one, w_one_f, load_sem.at[2]),
        pltpu.make_async_copy(w_two, w_two_f, load_sem.at[3]),
        pltpu.make_async_copy(labels, lab_v, load_sem.at[4]),
    ]
    for load in loads:
        load.start()
    for e in range(2):
        kept_copy(0, e).start()

    barrier = pltpu.get_barrier_semaphore()
    for dev in (pair, x_next, y_next):
        pl.semaphore_signal(barrier, inc=1, device_id=(dev,), device_id_type=MESH)
    acc_one[...] = jnp.zeros_like(acc_one)
    acc_two[...] = jnp.zeros_like(acc_two)
    grad_t[...] = jnp.zeros_like(grad_t)
    pl.semaphore_wait(barrier, 3)

    def piece(buf, s, e):
        blk, part = gather_place(s, e)
        return buf.at[blk, pl.ds(pl.multiple_of(part * quarter, quarter), quarter), :]

    def send_piece(ph, buf, s, e, to, dev):
        ref = piece(buf, s, e)
        at = 2 * to + e
        return remote(ref, ref, gather_send.at[ph, at], gather_recv.at[ph, at], dev)

    def send_own(ph, buf):
        for i in range(4):
            for e, dev in ((0, x_next), (1, y_next)):
                part = (i + 2 * e) % 4
                ref = buf.at[me, pl.ds(part * quarter, quarter), :]
                at = 2 * (4 + 2 * i) + e
                remote(ref, ref, gather_send.at[ph, at], gather_recv.at[ph, at], dev).start()

    def gather_step(ph, buf, s):
        for e in range(2):
            @pl.when(s >= 2)
            def _():
                send_piece(ph, buf, s, e, s, pair).wait_recv()

            @pl.when((s == 4) | (s == 6))
            def _():
                send_piece(ph, buf, s, e, s + 8, (y_next, x_next)[e]).start()

            @pl.when(s < 2)
            def _():
                send_piece(ph, buf, s, e, s + 2, pair).start()

            @pl.when((s >= 4) & (lax.rem(s, 2) == 0))
            def _():
                send_piece(ph, buf, s, e, s + 1, pair).start()

    def count_move(i):
        return remote(count.at[i], count_in.at[i], count_send.at[i], count_recv.at[i], (pair, x_next, y_next)[i])

    loads[0].wait()
    send_own(0, feats_all)
    for e in range(2):
        kept_copy(1, e).start()
        kept_copy(2, e).start()
    for load in loads[1:]:
        load.wait()
    count[0] = jnp.full((8, 128), jnp.sum(mask_v[...].astype(F32)), F32)
    count_move(0).start()
    w_one_b[...] = w_one_f[...].astype(BF16)
    w_one_t[...] = w_one_f[...].T.astype(BF16)
    w_two_t[...] = jnp.zeros_like(w_two_t)
    w_two_t[:classes, :] = w_two_f[...].astype(BF16)
    w_two_b[...] = w_two_t[...].astype(F32).T.astype(BF16)

    def step_one(s, carry):
        gather_step(0, feats_all, s)

        for i, when in enumerate((1, 12)):
            @pl.when(s == when)
            def _(i=i):
                count_move(i).wait_recv()
                count[i + 1] = count[i] + count_in[i]
                count_move(i + 1).start()

        kept = 1 - (s + 12) // 16
        slot = kept * (SLOTS + s) + (1 - kept) * lax.rem(s + 8, SLOTS)
        for e in range(2):
            adj_copy(gather_place(s, e), slot, e).wait()
        right = jnp.concatenate([piece(feats_all, s, e)[...] for e in range(2)], axis=0)
        for m in range(0, rows, M_CHUNK):
            at = pl.ds(m, M_CHUNK)
            acc_one[at, :] += _dot(adj_buf[slot, at, :], right)
        fetch(s - 4 + SLOTS)

        @pl.when(s == 0)
        def _():
            for e in range(2):
                kept_copy(3, e).start()

        @pl.when((s >= 1) & (s < 1 + SLOTS))
        def _():
            for e in range(2):
                slab_copy(s - 1, e).start()

        return carry

    lax.fori_loop(0, 16, step_one, 0)

    aggs_all[me] = acc_one[...].astype(BF16)
    send_own(1, aggs_all)

    def hidden_step(s, dst):
        for e in range(2):
            pre = _dot(piece(aggs_all, s, e)[...], w_one_b[...])
            dst[pl.ds(e * quarter, quarter), :] = jnp.maximum(pre, 0.0).astype(BF16)

    def step_two(s, now, then):
        @pl.when(s < 15)
        def _():
            gather_step(1, aggs_all, s + 1)

        kept = 1 - (s + 12) // 16
        slot = kept * (SLOTS + s) + (1 - kept) * lax.rem(s + 8, SLOTS)

        @pl.when(s >= 4)
        def _():
            for e in range(2):
                adj_copy(gather_place(s, e), slot, e).wait()

        hidden_step(jnp.minimum(s + 1, 15), then)
        right = now[...]
        for m in range(0, rows, M_TWO):
            at = pl.ds(m, M_TWO)
            acc_two[at, :] += _dot(adj_buf[slot, at, :], right)

        @pl.when(s >= 4)
        def _():
            fetch(s + 8 + SLOTS)

    def two_steps(i, carry):
        step_two(2 * i, hid, hid_next)
        step_two(2 * i + 1, hid_next, hid)
        return carry

    gather_step(1, aggs_all, jnp.int32(0))
    hidden_step(jnp.int32(0), hid)
    lax.fori_loop(0, 8, two_steps, 0)

    count_move(2).wait_recv()
    total = (count[2] + count_in[2])[0:1, 0:1]
    agg_two[...] = acc_two[...].astype(BF16)
    logits = _dot_nt(w_two_t[0:48, :], agg_two[...])[:classes, :]
    weight = mask_v[...].astype(F32)
    shifted = logits - jnp.max(logits, axis=0, keepdims=True)
    log_prob = shifted - jnp.log(jnp.sum(jnp.exp(shifted), axis=0, keepdims=True))
    onehot = (lax.broadcasted_iota(jnp.int32, (classes, rows), 0) == lab_v[...]).astype(F32)
    picked = jnp.sum(onehot * log_prob, axis=0, keepdims=True)
    loss_sum = -jnp.sum(weight * picked)
    grad_t[:classes, :] = (weight * (jnp.exp(log_prob) - onehot) / total).astype(BF16)
    back_t[...] = _dot(w_two_b[...], grad_t[...]).astype(BF16)

    def pair_move(u):
        at = lax.rem(u, 4)
        return remote(stage.at[at], from_pair.at[at], pair_send.at[at], pair_recv.at[u], pair)

    def chip_move(u):
        link = lax.rem(u, 2)
        dev = me + (1 - link) * to_x + link * to_y
        return remote(to_chip.at[u], from_chip.at[link, u // 2], chip_send.at[u], chip_recv.at[link, u // 2], dev)

    def finish(u):
        pair_move(u).wait_recv()
        both = own_part[lax.rem(u, 2)] + from_pair[lax.rem(u, 4)]

        @pl.when(u < 12)
        def _():
            to_chip[u] = both.astype(BF16)
            chip_move(u).start()
            pl.semaphore_signal(pair_free, inc=1, device_id=(pair,), device_id_type=MESH)

        @pl.when(u >= 12)
        def _():
            own_sums[u - 12] = both

    def step_three(u, carry):
        r = u + 24
        ring = 1 - u // 12
        kept = (1 - ring) * (u - 12)
        slots = [ring * lax.rem(r, SLOTS) + (1 - ring) * (SLOTS + 2 * (1 - e) + kept // 2) for e in range(2)]
        cols = [pl.multiple_of((ring * e + lax.rem(kept, 2)) * quarter, quarter) for e in range(2)]

        @pl.when(u >= 4)
        def _():
            pair_move(u).wait_send()
            pl.semaphore_wait(pair_free, 1)

        @pl.when(u < 12)
        def _():
            part_copy(r, 0).wait()

        stage[lax.rem(u, 4)] = _dot(back_t[...], adj_buf[slots[0], :, pl.ds(cols[0], quarter)])
        pair_move(u).start()

        @pl.when(u >= 1)
        def _():
            finish(u - 1)

        @pl.when(u < 12)
        def _():
            part_copy(r, 1).wait()

        own_part[lax.rem(u, 2)] = _dot(back_t[...], adj_buf[slots[1], :, pl.ds(cols[1], quarter)])
        fetch(r + SLOTS)
        return carry

    lax.fori_loop(0, 16, step_three, 0)
    finish(jnp.int32(15))
    for u in range(12, 16):
        pair_move(u).wait_send()

    part_two = _dot(grad_t[0:48, :], agg_two[...])
    small[0, 0:40, :] = part_two[0:classes, 0:128]
    small[0, 40:80, :] = part_two[0:classes, 128:256]
    small[0, 80:96, :] = jnp.full((16, 128), loss_sum, F32)

    def small_move(i):
        return remote(small.at[i], small_in.at[i], small_send.at[i], small_recv.at[i], (pair, x_next, y_next)[i])

    small_move(0).start()
    pre_t[...] = _dot_nt(w_one_t[...], aggs_all[me])

    small_move(0).wait_recv()
    small[1] = small[0] + small_in[0]
    small_move(1).start()

    relays = []
    for k in range(2):
        for link in range(2):
            chip_move(2 * k + link).wait_recv()
            move = remote(from_chip.at[link, k], from_chip.at[1 - link, 6 + k], relay_send.at[link, k],
                          chip_recv.at[1 - link, 6 + k], (y_next, x_next)[link])
            move.start()
            relays.append(move)

    for j in range(4):
        for link in range(2):
            chip_move(4 + 2 * j + link).wait_recv()
            own_sums[j] += from_chip[link, 2 + j].astype(F32)
    small_move(1).wait_recv()
    small[2] = small[1] + small_in[1]
    small_move(2).start()
    red_one = jnp.zeros((256, 128), F32)
    for k in range(2):
        for link in range(2):
            j = 2 * (1 - link) + k
            relays[2 * k + 1 - link].wait_recv()
            d_hidden = own_sums[j] + from_chip[link, 6 + k].astype(F32)
            keep = pre_t[:, pl.ds(j * quarter, quarter)] > 0.0
            grad_one = jnp.where(keep, d_hidden, 0.0).astype(BF16)
            red_one += _dot(grad_one, aggs_all[me, pl.ds(j * quarter, quarter), :])
    red[...] = red_one

    n_half = red.shape[0] // 2
    n_part = n_half // 2
    mine = pl.multiple_of(core * n_half, 8)
    other = pl.multiple_of((1 - core) * n_half, 8)

    move = remote(red.at[pl.ds(other, n_half)], red_pair, red_send.at[0], red_recv.at[0], pair)
    move.start()
    move.wait_recv()
    red_link[...] = red[pl.ds(mine, n_half), :] + red_pair[...]
    moves = [
        remote(red_link.at[pl.ds(i * n_part, n_part)], red_next.at[pl.ds(i * n_part, n_part)],
               red_send.at[1 + i], red_recv.at[1 + i], (x_next, y_next)[i])
        for i in range(2)
    ]
    for m in moves:
        m.start()
    for m in moves:
        m.wait_recv()
    red_pair2 = red_link[...] + red_next[...]
    red_last[0] = red_pair2
    lasts = [
        remote(red_last.at[0, pl.ds(i * n_part, n_part)], red_last.at[1, pl.ds(i * n_part, n_part)],
               red_send.at[3 + i], red_recv.at[3 + i], (y_next, x_next)[i])
        for i in range(2)
    ]
    for m in lasts:
        m.start()
    for m in lasts:
        m.wait_recv()
    red_out[pl.ds(mine, n_half), :] = red_last[0] + red_last[1]
    ref = red_out.at[pl.ds(mine, n_half)]
    back = remote(ref, ref, red_send.at[5], red_recv.at[5], pair)
    back.start()
    ref_in = red_out.at[pl.ds(other, n_half)]
    remote(ref_in, ref_in, red_send.at[5], red_recv.at[5], pair).wait_recv()

    small_move(2).wait_recv()
    summed = small[2] + small_in[2]
    out[0:256, :] = red_out[...]
    out[256:336, :] = summed[0:80, :]
    out[336:352, :] = summed[80:96, :] / total

    move.wait_send()
    for m in moves + lasts + [back]:
        m.wait_send()
    for i in range(3):
        count_move(i).wait_send()
        small_move(i).wait_send()
    for ph, buf in ((0, feats_all), (1, aggs_all)):
        for to in range(2, 16):
            for e in range(2):
                send_piece(ph, buf, to, e, to, pair).wait_send()
    for u in range(12):
        chip_move(u).wait_send()
    for relay in relays:
        relay.wait_send()


def _finish(sums, out_loss, out_one, out_two):
    classes = out_two.shape[0]
    out_one[...] = sums[0:256, :].T
    out_two[:, 0:128] = sums[256:256 + classes, :]
    out_two[:, 128:256] = sums[256 + classes:256 + 2 * classes, :]
    out_loss[...] = sums[336:337, 0:1]


def solution(mesh):
    def step(adj, feat, w_one, w_two, labels, mask):
        rows, nodes = adj.shape
        feat_dim, hidden = w_one.shape
        classes = w_two.shape[1]
        parts = nodes // rows
        any_spec = pl.BlockSpec(memory_space=pltpu.HBM)
        vmem = pl.BlockSpec(memory_space=pltpu.VMEM)
        quarter = rows // 4
        scratch = [
            pltpu.VMEM((parts, rows, feat_dim), BF16),
            pltpu.VMEM((parts, rows, feat_dim), BF16),
            pltpu.VMEM((rows // 2, hidden), BF16),
            pltpu.VMEM((rows // 2, hidden), BF16),
            pltpu.VMEM((rows, feat_dim), F32),
            pltpu.VMEM((rows, hidden), F32),
            pltpu.VMEM((rows, hidden), BF16),
            pltpu.VMEM((hidden, rows), BF16),
            pltpu.VMEM((128, rows), BF16),
            pltpu.VMEM((hidden, rows), F32),
            pltpu.VMEM((2, hidden, quarter), F32),
            pltpu.VMEM((4, hidden, quarter), F32),
            pltpu.VMEM((4, hidden, quarter), F32),
            pltpu.VMEM((4, hidden, quarter), F32),
            pltpu.VMEM((12, hidden, quarter), BF16),
            pltpu.VMEM((2, 8, hidden, quarter), BF16),
            pltpu.VMEM((SLOTS + 4, rows, rows // 2), BF16),
            pltpu.VMEM((feat_dim, hidden), F32),
            pltpu.VMEM((classes, hidden), F32),
            pltpu.VMEM((feat_dim, hidden), BF16),
            pltpu.VMEM((hidden, feat_dim), BF16),
            pltpu.VMEM((hidden, 128), BF16),
            pltpu.VMEM((128, hidden), BF16),
            pltpu.VMEM((1, rows), jnp.int32),
            pltpu.VMEM((1, rows), jnp.int32),
            pltpu.VMEM((3, 8, 128), F32),
            pltpu.VMEM((3, 8, 128), F32),
            pltpu.VMEM((256, 128), F32),
            pltpu.VMEM((128, 128), F32),
            pltpu.VMEM((128, 128), F32),
            pltpu.VMEM((128, 128), F32),
            pltpu.VMEM((2, 128, 128), F32),
            pltpu.VMEM((256, 128), F32),
            pltpu.VMEM((3, 96, 128), F32),
            pltpu.VMEM((3, 96, 128), F32),
            pltpu.SemaphoreType.DMA((SLOTS + 4, 2)),
            pltpu.SemaphoreType.DMA((5,)),
            pltpu.SemaphoreType.DMA((2, 32)),
            pltpu.SemaphoreType.DMA((2, 32)),
            pltpu.SemaphoreType.DMA((3,)),
            pltpu.SemaphoreType.DMA((3,)),
            pltpu.SemaphoreType.DMA((4,)),
            pltpu.SemaphoreType.DMA((16,)),
            pltpu.SemaphoreType.REGULAR,
            pltpu.SemaphoreType.DMA((12,)),
            pltpu.SemaphoreType.DMA((2, 8)),
            pltpu.SemaphoreType.DMA((6,)),
            pltpu.SemaphoreType.DMA((6,)),
            pltpu.SemaphoreType.DMA((3,)),
            pltpu.SemaphoreType.DMA((3,)),
            pltpu.SemaphoreType.DMA((2, 2)),
        ]
        sums = pl.pallas_call(
            _kernel,
            out_shape=jax.ShapeDtypeStruct((352, 128), F32),
            in_specs=[any_spec] * 6,
            out_specs=vmem,
            scratch_shapes=scratch,
            compiler_params=pltpu.CompilerParams(
                collective_id=0, has_side_effects=True, vmem_limit_bytes=67_000_000),
            name="gcn_step",
        )(adj, feat, w_one, w_two.T, labels.reshape(1, rows), mask.reshape(1, rows))
        loss, dw_one, dw_two_t = pl.pallas_call(
            _finish,
            out_shape=(
                jax.ShapeDtypeStruct((1, 1), F32),
                jax.ShapeDtypeStruct((feat_dim, hidden), F32),
                jax.ShapeDtypeStruct((classes, hidden), F32),
            ),
            in_specs=[vmem],
            out_specs=(vmem, vmem, vmem),
            name="gcn_finish",
        )(sums)
        return loss.reshape(1), dw_one, dw_two_t.T

    return jax.shard_map(
        step,
        mesh=mesh,
        in_specs=(P(AXIS, None), P(AXIS, None), P(None, None), P(None, None), P(AXIS), P(AXIS)),
        out_specs=(P(None), P(None, None), P(None, None)),
        check_vma=False,
    )
```

```python
import jax
import jax.numpy as jnp
from jax import lax
from jax.experimental import pallas as pl
from jax.experimental.pallas import tpu as pltpu
from jax.sharding import PartitionSpec as P

AXIS = "nodes"
MESH = pl.DeviceIdType.MESH
F32 = jnp.float32
BF16 = jnp.bfloat16

SLOTS = 3
M_CHUNK = 512
M_TWO = 512


def _dot(a, b):
    return jnp.dot(a, b, preferred_element_type=F32)


def _dot_nt(a, b):
    return lax.dot_general(a, b, (((1,), (1,)), ((), ())), preferred_element_type=F32)


def _kernel(
    adj, feat, w_one, w_two, labels, mask,
    out,
    feats_all, aggs_all, hid, hid_next, acc_one, acc_two, agg_two, back_t, grad_t, pre_t,
    own_part, own_sums, stage, from_pair, to_chip, from_chip, adj_buf,
    w_one_f, w_two_f, w_one_b, w_one_t, w_two_b, w_two_t, lab_v, mask_v, count, count_in,
    red, red_pair, red_link, red_next, red_last, red_out, small, small_in,
    adj_sem, load_sem, gather_send, gather_recv, count_send, count_recv,
    pair_send, pair_recv, pair_free, chip_send, chip_recv, red_send, red_recv, small_send, small_recv, relay_send,
):
    rows = feat.shape[0]
    quarter = rows // 4
    classes = w_two.shape[0]
    me = lax.axis_index(AXIS)
    core, chip_x, chip_y = lax.rem(me, 2), lax.rem(me // 2, 2), me // 4
    to_pair, to_x, to_y = 1 - 2 * core, 2 - 4 * chip_x, 4 - 8 * chip_y
    pair, x_next, y_next = me + to_pair, me + to_x, me + to_y

    def remote(src, dst, send, recv, dev):
        return pltpu.make_async_remote_copy(
            src_ref=src, dst_ref=dst, send_sem=send, recv_sem=recv, device_id=(dev,), device_id_type=MESH)

    def gather_place(s, e):
        low = 1 - (s + 12) // 16
        far = s // 12
        near = 1 - low - far
        flip = low * (s // 2) + (1 - low) * lax.rem(s, 2)
        blk = me + flip * to_pair + (near * (1 - e) + far) * to_x + (near * e + far) * to_y
        part = (low * (2 * lax.rem(s, 2) + e) + near * lax.rem(s // 2 + 2 + 2 * e, 4) + far * (s // 2 - 6 + 2 * e))
        return blk, part

    def reduce_place(u):
        own = u // 12
        diag = 1 - (u + 12) // 16
        near = 1 - own - diag
        link = lax.rem(u, 2)
        nx = diag + near * (1 - link)
        ny = diag + near * link
        part = own * (u - 12) + diag * (2 * link + u // 2) + near * (u // 2 - 2)
        return me + nx * to_x + ny * to_y, part

    def adj_copy(place, slot, e):
        blk, part = place
        col = pl.multiple_of(blk * rows + part * quarter, quarter)
        return pltpu.make_async_copy(
            adj.at[:, pl.ds(col, quarter)], adj_buf.at[slot, :, pl.ds(e * quarter, quarter)], adj_sem.at[slot, e])

    def kept_copy(s, e):
        return adj_copy(gather_place(s, e), SLOTS + s, e)

    def slab_copy(r, e):
        return adj_copy(gather_place(lax.rem(r, 12) + 4, e), lax.rem(r, SLOTS), e)

    def part_copy(r, e):
        blk, part = reduce_place(r - 24)
        return adj_copy((blk + to_pair * (1 - e), part), lax.rem(r, SLOTS), e)

    def fetch(r):
        @pl.when((r >= SLOTS) & (r < 24))
        def _():
            for e in range(2):
                slab_copy(r, e).start()

        @pl.when((r >= 24) & (r < 36))
        def _():
            for e in range(2):
                part_copy(r, e).start()

    loads = [
        pltpu.make_async_copy(feat, feats_all.at[me], load_sem.at[0]),
        pltpu.make_async_copy(mask, mask_v, load_sem.at[1]),
        pltpu.make_async_copy(w_one, w_one_f, load_sem.at[2]),
        pltpu.make_async_copy(w_two, w_two_f, load_sem.at[3]),
        pltpu.make_async_copy(labels, lab_v, load_sem.at[4]),
    ]
    for load in loads:
        load.start()
    for e in range(2):
        kept_copy(0, e).start()

    barrier = pltpu.get_barrier_semaphore()
    for dev in (pair, x_next, y_next):
        pl.semaphore_signal(barrier, inc=1, device_id=(dev,), device_id_type=MESH)
    acc_one[...] = jnp.zeros_like(acc_one)
    acc_two[...] = jnp.zeros_like(acc_two)
    grad_t[...] = jnp.zeros_like(grad_t)
    pl.semaphore_wait(barrier, 3)

    def piece(buf, s, e):
        blk, part = gather_place(s, e)
        return buf.at[blk, pl.ds(pl.multiple_of(part * quarter, quarter), quarter), :]

    def send_piece(ph, buf, s, e, to, dev):
        ref = piece(buf, s, e)
        at = 2 * to + e
        return remote(ref, ref, gather_send.at[ph, at], gather_recv.at[ph, at], dev)

    def send_own(ph, buf):
        for i in range(4):
            for e, dev in ((0, x_next), (1, y_next)):
                part = (i + 2 * e) % 4
                ref = buf.at[me, pl.ds(part * quarter, quarter), :]
                at = 2 * (4 + 2 * i) + e
                remote(ref, ref, gather_send.at[ph, at], gather_recv.at[ph, at], dev).start()

    def gather_step(ph, buf, s):
        for e in range(2):
            @pl.when(s >= 2)
            def _():
                send_piece(ph, buf, s, e, s, pair).wait_recv()

            @pl.when((s == 4) | (s == 6))
            def _():
                send_piece(ph, buf, s, e, s + 8, (y_next, x_next)[e]).start()

            @pl.when(s < 2)
            def _():
                send_piece(ph, buf, s, e, s + 2, pair).start()

            @pl.when((s >= 4) & (lax.rem(s, 2) == 0))
            def _():
                send_piece(ph, buf, s, e, s + 1, pair).start()

    def count_move(i):
        return remote(count.at[i], count_in.at[i], count_send.at[i], count_recv.at[i], (pair, x_next, y_next)[i])

    loads[0].wait()
    send_own(0, feats_all)
    for e in range(2):
        kept_copy(1, e).start()
        kept_copy(2, e).start()
    for load in loads[1:]:
        load.wait()
    count[0] = jnp.full((8, 128), jnp.sum(mask_v[...].astype(F32)), F32)
    count_move(0).start()
    w_one_b[...] = w_one_f[...].astype(BF16)
    w_one_t[...] = w_one_f[...].T.astype(BF16)
    w_two_t[...] = jnp.zeros_like(w_two_t)
    w_two_t[:classes, :] = w_two_f[...].astype(BF16)
    w_two_b[...] = w_two_t[...].astype(F32).T.astype(BF16)

    def step_one(s, carry):
        gather_step(0, feats_all, s)

        for i, when in enumerate((1, 12)):
            @pl.when(s == when)
            def _(i=i):
                count_move(i).wait_recv()
                count[i + 1] = count[i] + count_in[i]
                count_move(i + 1).start()

        kept = 1 - (s + 12) // 16
        slot = kept * (SLOTS + s) + (1 - kept) * lax.rem(s + 8, SLOTS)
        for e in range(2):
            adj_copy(gather_place(s, e), slot, e).wait()
        right = jnp.concatenate([piece(feats_all, s, e)[...] for e in range(2)], axis=0)
        for m in range(0, rows, M_CHUNK):
            at = pl.ds(m, M_CHUNK)
            acc_one[at, :] += _dot(adj_buf[slot, at, :], right)
        fetch(s - 4 + SLOTS)

        @pl.when(s == 0)
        def _():
            for e in range(2):
                kept_copy(3, e).start()

        @pl.when((s >= 1) & (s < 1 + SLOTS))
        def _():
            for e in range(2):
                slab_copy(s - 1, e).start()

        return carry

    lax.fori_loop(0, 16, step_one, 0)

    aggs_all[me] = acc_one[...].astype(BF16)
    send_own(1, aggs_all)

    def hidden_step(s, dst):
        for e in range(2):
            pre = _dot(piece(aggs_all, s, e)[...], w_one_b[...])
            dst[pl.ds(e * quarter, quarter), :] = jnp.maximum(pre, 0.0).astype(BF16)

    def step_two(s, now, then):
        @pl.when(s < 15)
        def _():
            gather_step(1, aggs_all, s + 1)

        kept = 1 - (s + 12) // 16
        slot = kept * (SLOTS + s) + (1 - kept) * lax.rem(s + 8, SLOTS)

        @pl.when(s >= 4)
        def _():
            for e in range(2):
                adj_copy(gather_place(s, e), slot, e).wait()

        hidden_step(jnp.minimum(s + 1, 15), then)
        right = now[...]
        for m in range(0, rows, M_TWO):
            at = pl.ds(m, M_TWO)
            acc_two[at, :] += _dot(adj_buf[slot, at, :], right)

        @pl.when(s >= 4)
        def _():
            fetch(s + 8 + SLOTS)

    def two_steps(i, carry):
        step_two(2 * i, hid, hid_next)
        step_two(2 * i + 1, hid_next, hid)
        return carry

    gather_step(1, aggs_all, jnp.int32(0))
    hidden_step(jnp.int32(0), hid)
    lax.fori_loop(0, 8, two_steps, 0)

    count_move(2).wait_recv()
    total = (count[2] + count_in[2])[0:1, 0:1]
    agg_two[...] = acc_two[...].astype(BF16)
    logits = _dot_nt(w_two_t[0:48, :], agg_two[...])[:classes, :]
    weight = mask_v[...].astype(F32)
    shifted = logits - jnp.max(logits, axis=0, keepdims=True)
    log_prob = shifted - jnp.log(jnp.sum(jnp.exp(shifted), axis=0, keepdims=True))
    onehot = (lax.broadcasted_iota(jnp.int32, (classes, rows), 0) == lab_v[...]).astype(F32)
    picked = jnp.sum(onehot * log_prob, axis=0, keepdims=True)
    loss_sum = -jnp.sum(weight * picked)
    grad_t[:classes, :] = (weight * (jnp.exp(log_prob) - onehot) / total).astype(BF16)
    back_t[...] = _dot(w_two_b[...], grad_t[...]).astype(BF16)

    def pair_move(u):
        at = lax.rem(u, 4)
        return remote(stage.at[at], from_pair.at[at], pair_send.at[at], pair_recv.at[u], pair)

    def chip_move(u):
        link = lax.rem(u, 2)
        dev = me + (1 - link) * to_x + link * to_y
        return remote(to_chip.at[u], from_chip.at[link, u // 2], chip_send.at[u], chip_recv.at[link, u // 2], dev)

    def finish(u):
        pair_move(u).wait_recv()
        both = own_part[lax.rem(u, 2)] + from_pair[lax.rem(u, 4)]

        @pl.when(u < 12)
        def _():
            to_chip[u] = both.astype(BF16)
            chip_move(u).start()
            pl.semaphore_signal(pair_free, inc=1, device_id=(pair,), device_id_type=MESH)

        @pl.when(u >= 12)
        def _():
            own_sums[u - 12] = both

    def make_part(u, which):
        r = u + 24
        ring = 1 - u // 12
        kept = (1 - ring) * (u - 12)
        slot = ring * lax.rem(r, SLOTS) + (1 - ring) * (SLOTS + 2 * (1 - which) + kept // 2)
        col = pl.multiple_of((ring * which + lax.rem(kept, 2)) * quarter, quarter)

        @pl.when(u < 12)
        def _():
            part_copy(r, which).wait()

        part = _dot(back_t[...], adj_buf[slot, :, pl.ds(col, quarter)])
        if which == 0:
            stage[lax.rem(u, 4)] = part
            pair_move(u).start()
        else:
            own_part[lax.rem(u, 2)] = part
            fetch(r + SLOTS)

    def step_three(u, carry):
        @pl.when(u >= 4)
        def _():
            pair_move(u).wait_send()
            pl.semaphore_wait(pair_free, 1)

        make_part(u, 0)

        @pl.when(u >= 3)
        def _():
            finish(u - 1)

        make_part(u, 1)
        return carry

    first, second = jnp.int32(0), jnp.int32(1)
    make_part(first, 0)
    make_part(second, 0)
    make_part(first, 1)
    finish(first)
    make_part(second, 1)
    finish(second)
    lax.fori_loop(2, 16, step_three, 0)
    finish(jnp.int32(15))
    for u in range(12, 16):
        pair_move(u).wait_send()

    part_two = _dot(grad_t[0:48, :], agg_two[...])
    small[0, 0:40, :] = part_two[0:classes, 0:128]
    small[0, 40:80, :] = part_two[0:classes, 128:256]
    small[0, 80:96, :] = jnp.full((16, 128), loss_sum, F32)

    def small_move(i):
        return remote(small.at[i], small_in.at[i], small_send.at[i], small_recv.at[i], (pair, x_next, y_next)[i])

    small_move(0).start()
    pre_t[...] = _dot_nt(w_one_t[...], aggs_all[me])

    small_move(0).wait_recv()
    small[1] = small[0] + small_in[0]
    small_move(1).start()

    relays = []
    for k in range(2):
        for link in range(2):
            chip_move(2 * k + link).wait_recv()
            move = remote(from_chip.at[link, k], from_chip.at[1 - link, 6 + k], relay_send.at[link, k],
                          chip_recv.at[1 - link, 6 + k], (y_next, x_next)[link])
            move.start()
            relays.append(move)

    for j in range(4):
        for link in range(2):
            chip_move(4 + 2 * j + link).wait_recv()
            own_sums[j] += from_chip[link, 2 + j].astype(F32)
    small_move(1).wait_recv()
    small[2] = small[1] + small_in[1]
    small_move(2).start()
    red_one = jnp.zeros((256, 128), F32)
    for k in range(2):
        for link in range(2):
            j = 2 * (1 - link) + k
            relays[2 * k + 1 - link].wait_recv()
            d_hidden = own_sums[j] + from_chip[link, 6 + k].astype(F32)
            keep = pre_t[:, pl.ds(j * quarter, quarter)] > 0.0
            grad_one = jnp.where(keep, d_hidden, 0.0).astype(BF16)
            red_one += _dot(grad_one, aggs_all[me, pl.ds(j * quarter, quarter), :])
    red[...] = red_one

    n_half = red.shape[0] // 2
    n_part = n_half // 2
    mine = pl.multiple_of(core * n_half, 8)
    other = pl.multiple_of((1 - core) * n_half, 8)

    move = remote(red.at[pl.ds(other, n_half)], red_pair, red_send.at[0], red_recv.at[0], pair)
    move.start()
    move.wait_recv()
    red_link[...] = red[pl.ds(mine, n_half), :] + red_pair[...]
    moves = [
        remote(red_link.at[pl.ds(i * n_part, n_part)], red_next.at[pl.ds(i * n_part, n_part)],
               red_send.at[1 + i], red_recv.at[1 + i], (x_next, y_next)[i])
        for i in range(2)
    ]
    for m in moves:
        m.start()
    for m in moves:
        m.wait_recv()
    red_pair2 = red_link[...] + red_next[...]
    red_last[0] = red_pair2
    lasts = [
        remote(red_last.at[0, pl.ds(i * n_part, n_part)], red_last.at[1, pl.ds(i * n_part, n_part)],
               red_send.at[3 + i], red_recv.at[3 + i], (y_next, x_next)[i])
        for i in range(2)
    ]
    for m in lasts:
        m.start()
    for m in lasts:
        m.wait_recv()
    red_out[pl.ds(mine, n_half), :] = red_last[0] + red_last[1]
    ref = red_out.at[pl.ds(mine, n_half)]
    back = remote(ref, ref, red_send.at[5], red_recv.at[5], pair)
    back.start()
    ref_in = red_out.at[pl.ds(other, n_half)]
    remote(ref_in, ref_in, red_send.at[5], red_recv.at[5], pair).wait_recv()

    small_move(2).wait_recv()
    summed = small[2] + small_in[2]
    out[0:256, :] = red_out[...]
    out[256:336, :] = summed[0:80, :]
    out[336:352, :] = summed[80:96, :] / total

    move.wait_send()
    for m in moves + lasts + [back]:
        m.wait_send()
    for i in range(3):
        count_move(i).wait_send()
        small_move(i).wait_send()
    for ph, buf in ((0, feats_all), (1, aggs_all)):
        for to in range(2, 16):
            for e in range(2):
                send_piece(ph, buf, to, e, to, pair).wait_send()
    for u in range(12):
        chip_move(u).wait_send()
    for relay in relays:
        relay.wait_send()


def _finish(sums, out_loss, out_one, out_two):
    classes = out_two.shape[0]
    out_one[...] = sums[0:256, :].T
    out_two[:, 0:128] = sums[256:256 + classes, :]
    out_two[:, 128:256] = sums[256 + classes:256 + 2 * classes, :]
    out_loss[...] = sums[336:337, 0:1]


def solution(mesh):
    def step(adj, feat, w_one, w_two, labels, mask):
        rows, nodes = adj.shape
        feat_dim, hidden = w_one.shape
        classes = w_two.shape[1]
        parts = nodes // rows
        any_spec = pl.BlockSpec(memory_space=pltpu.HBM)
        vmem = pl.BlockSpec(memory_space=pltpu.VMEM)
        quarter = rows // 4
        scratch = [
            pltpu.VMEM((parts, rows, feat_dim), BF16),
            pltpu.VMEM((parts, rows, feat_dim), BF16),
            pltpu.VMEM((rows // 2, hidden), BF16),
            pltpu.VMEM((rows // 2, hidden), BF16),
            pltpu.VMEM((rows, feat_dim), F32),
            pltpu.VMEM((rows, hidden), F32),
            pltpu.VMEM((rows, hidden), BF16),
            pltpu.VMEM((hidden, rows), BF16),
            pltpu.VMEM((128, rows), BF16),
            pltpu.VMEM((hidden, rows), F32),
            pltpu.VMEM((2, hidden, quarter), F32),
            pltpu.VMEM((4, hidden, quarter), F32),
            pltpu.VMEM((4, hidden, quarter), F32),
            pltpu.VMEM((4, hidden, quarter), F32),
            pltpu.VMEM((12, hidden, quarter), BF16),
            pltpu.VMEM((2, 8, hidden, quarter), BF16),
            pltpu.VMEM((SLOTS + 4, rows, rows // 2), BF16),
            pltpu.VMEM((feat_dim, hidden), F32),
            pltpu.VMEM((classes, hidden), F32),
            pltpu.VMEM((feat_dim, hidden), BF16),
            pltpu.VMEM((hidden, feat_dim), BF16),
            pltpu.VMEM((hidden, 128), BF16),
            pltpu.VMEM((128, hidden), BF16),
            pltpu.VMEM((1, rows), jnp.int32),
            pltpu.VMEM((1, rows), jnp.int32),
            pltpu.VMEM((3, 8, 128), F32),
            pltpu.VMEM((3, 8, 128), F32),
            pltpu.VMEM((256, 128), F32),
            pltpu.VMEM((128, 128), F32),
            pltpu.VMEM((128, 128), F32),
            pltpu.VMEM((128, 128), F32),
            pltpu.VMEM((2, 128, 128), F32),
            pltpu.VMEM((256, 128), F32),
            pltpu.VMEM((3, 96, 128), F32),
            pltpu.VMEM((3, 96, 128), F32),
            pltpu.SemaphoreType.DMA((SLOTS + 4, 2)),
            pltpu.SemaphoreType.DMA((5,)),
            pltpu.SemaphoreType.DMA((2, 32)),
            pltpu.SemaphoreType.DMA((2, 32)),
            pltpu.SemaphoreType.DMA((3,)),
            pltpu.SemaphoreType.DMA((3,)),
            pltpu.SemaphoreType.DMA((4,)),
            pltpu.SemaphoreType.DMA((16,)),
            pltpu.SemaphoreType.REGULAR,
            pltpu.SemaphoreType.DMA((12,)),
            pltpu.SemaphoreType.DMA((2, 8)),
            pltpu.SemaphoreType.DMA((6,)),
            pltpu.SemaphoreType.DMA((6,)),
            pltpu.SemaphoreType.DMA((3,)),
            pltpu.SemaphoreType.DMA((3,)),
            pltpu.SemaphoreType.DMA((2, 2)),
        ]
        sums = pl.pallas_call(
            _kernel,
            out_shape=jax.ShapeDtypeStruct((352, 128), F32),
            in_specs=[any_spec] * 6,
            out_specs=vmem,
            scratch_shapes=scratch,
            compiler_params=pltpu.CompilerParams(
                collective_id=0, has_side_effects=True, vmem_limit_bytes=67_000_000),
            name="gcn_step",
        )(adj, feat, w_one, w_two.T, labels.reshape(1, rows), mask.reshape(1, rows))
        loss, dw_one, dw_two_t = pl.pallas_call(
            _finish,
            out_shape=(
                jax.ShapeDtypeStruct((1, 1), F32),
                jax.ShapeDtypeStruct((feat_dim, hidden), F32),
                jax.ShapeDtypeStruct((classes, hidden), F32),
            ),
            in_specs=[vmem],
            out_specs=(vmem, vmem, vmem),
            name="gcn_finish",
        )(sums)
        return loss.reshape(1), dw_one, dw_two_t.T

    return jax.shard_map(
        step,
        mesh=mesh,
        in_specs=(P(AXIS, None), P(AXIS, None), P(None, None), P(None, None), P(AXIS), P(AXIS)),
        out_specs=(P(None), P(None, None), P(None, None)),
        check_vma=False,
    )
```

```python
import jax
import jax.numpy as jnp
from jax import lax
from jax.experimental import pallas as pl
from jax.experimental.pallas import tpu as pltpu
from jax.sharding import PartitionSpec as P

AXIS = "nodes"
MESH = pl.DeviceIdType.MESH
F32 = jnp.float32
BF16 = jnp.bfloat16

SLOTS = 3
M_CHUNK = 512
M_TWO = 512


def _dot(a, b):
    return jnp.dot(a, b, preferred_element_type=F32)


def _dot_nt(a, b):
    return lax.dot_general(a, b, (((1,), (1,)), ((), ())), preferred_element_type=F32)


def _kernel(
    adj, feat, w_one, w_two, labels, mask,
    out,
    feats_all, aggs_all, hid, hid_next, acc_one, acc_two, agg_two, back_t, grad_t, pre_t,
    own_part, own_sums, stage, from_pair, to_chip, from_chip, adj_buf,
    w_one_f, w_two_f, w_one_b, w_one_t, w_two_b, w_two_t, lab_v, mask_v, count, count_in,
    red, red_pair, red_link, red_next, red_last, red_out, small, small_in,
    adj_sem, load_sem, gather_send, gather_recv, count_send, count_recv,
    pair_send, pair_recv, pair_free, chip_send, chip_recv, red_send, red_recv, small_send, small_recv, relay_send,
):
    rows = feat.shape[0]
    quarter = rows // 4
    classes = w_two.shape[0]
    me = lax.axis_index(AXIS)
    core, chip_x, chip_y = lax.rem(me, 2), lax.rem(me // 2, 2), me // 4
    to_pair, to_x, to_y = 1 - 2 * core, 2 - 4 * chip_x, 4 - 8 * chip_y
    pair, x_next, y_next = me + to_pair, me + to_x, me + to_y

    def remote(src, dst, send, recv, dev):
        return pltpu.make_async_remote_copy(
            src_ref=src, dst_ref=dst, send_sem=send, recv_sem=recv, device_id=(dev,), device_id_type=MESH)

    def gather_place(s, e):
        low = 1 - (s + 12) // 16
        far = s // 12
        near = 1 - low - far
        flip = low * (s // 2) + (1 - low) * lax.rem(s, 2)
        blk = me + flip * to_pair + (near * (1 - e) + far) * to_x + (near * e + far) * to_y
        part = (low * (2 * lax.rem(s, 2) + e) + near * lax.rem(s // 2 + 2 + 2 * e, 4) + far * (s // 2 - 6 + 2 * e))
        return blk, part

    def reduce_place(u):
        own = u // 12
        diag = 1 - (u + 12) // 16
        near = 1 - own - diag
        link = lax.rem(u, 2)
        nx = diag + near * (1 - link)
        ny = diag + near * link
        part = own * (u - 12) + diag * (2 * link + u // 2) + near * (u // 2 - 2)
        return me + nx * to_x + ny * to_y, part

    def adj_copy(place, slot, e):
        blk, part = place
        col = pl.multiple_of(blk * rows + part * quarter, quarter)
        return pltpu.make_async_copy(
            adj.at[:, pl.ds(col, quarter)], adj_buf.at[slot, :, pl.ds(e * quarter, quarter)], adj_sem.at[slot, e])

    def kept_copy(s, e):
        return adj_copy(gather_place(s, e), SLOTS + s, e)

    def slab_copy(r, e):
        return adj_copy(gather_place(lax.rem(r, 12) + 4, e), lax.rem(r, SLOTS), e)

    def part_copy(r, e):
        blk, part = reduce_place(r - 24)
        return adj_copy((blk + to_pair * (1 - e), part), lax.rem(r, SLOTS), e)

    def fetch(r):
        @pl.when((r >= SLOTS) & (r < 24))
        def _():
            for e in range(2):
                slab_copy(r, e).start()

        @pl.when((r >= 24) & (r < 36))
        def _():
            for e in range(2):
                part_copy(r, e).start()

    loads = [
        pltpu.make_async_copy(feat, feats_all.at[me], load_sem.at[0]),
        pltpu.make_async_copy(mask, mask_v, load_sem.at[1]),
        pltpu.make_async_copy(w_one, w_one_f, load_sem.at[2]),
        pltpu.make_async_copy(w_two, w_two_f, load_sem.at[3]),
        pltpu.make_async_copy(labels, lab_v, load_sem.at[4]),
    ]
    for load in loads:
        load.start()
    for e in range(2):
        kept_copy(0, e).start()

    barrier = pltpu.get_barrier_semaphore()
    for dev in (pair, x_next, y_next):
        pl.semaphore_signal(barrier, inc=1, device_id=(dev,), device_id_type=MESH)
    acc_one[...] = jnp.zeros_like(acc_one)
    acc_two[...] = jnp.zeros_like(acc_two)
    grad_t[...] = jnp.zeros_like(grad_t)
    pl.semaphore_wait(barrier, 3)

    def piece(buf, s, e):
        blk, part = gather_place(s, e)
        return buf.at[blk, pl.ds(pl.multiple_of(part * quarter, quarter), quarter), :]

    def send_piece(ph, buf, s, e, to, dev):
        ref = piece(buf, s, e)
        at = 2 * to + e
        return remote(ref, ref, gather_send.at[ph, at], gather_recv.at[ph, at], dev)

    def send_own(ph, buf):
        for i in range(4):
            for e, dev in ((0, x_next), (1, y_next)):
                part = (i + 2 * e) % 4
                ref = buf.at[me, pl.ds(part * quarter, quarter), :]
                at = 2 * (4 + 2 * i) + e
                remote(ref, ref, gather_send.at[ph, at], gather_recv.at[ph, at], dev).start()

    def gather_step(ph, buf, s):
        for e in range(2):
            @pl.when(s >= 2)
            def _():
                send_piece(ph, buf, s, e, s, pair).wait_recv()

            @pl.when((s == 4) | (s == 6))
            def _():
                send_piece(ph, buf, s, e, s + 8, (y_next, x_next)[e]).start()

            @pl.when(s < 2)
            def _():
                send_piece(ph, buf, s, e, s + 2, pair).start()

            @pl.when((s >= 4) & (lax.rem(s, 2) == 0))
            def _():
                send_piece(ph, buf, s, e, s + 1, pair).start()

    def count_move(i):
        return remote(count.at[i], count_in.at[i], count_send.at[i], count_recv.at[i], (pair, x_next, y_next)[i])

    loads[0].wait()
    send_own(0, feats_all)
    for e in range(2):
        kept_copy(1, e).start()
        kept_copy(2, e).start()
    for load in loads[1:]:
        load.wait()
    count[0] = jnp.full((8, 128), jnp.sum(mask_v[...].astype(F32)), F32)
    count_move(0).start()
    w_one_b[...] = w_one_f[...].astype(BF16)
    w_one_t[...] = w_one_f[...].T.astype(BF16)
    w_two_t[...] = jnp.zeros_like(w_two_t)
    w_two_t[:classes, :] = w_two_f[...].astype(BF16)
    w_two_b[...] = w_two_t[...].astype(F32).T.astype(BF16)

    def step_one(s, carry):
        gather_step(0, feats_all, s)

        for i, when in enumerate((1, 12)):
            @pl.when(s == when)
            def _(i=i):
                count_move(i).wait_recv()
                count[i + 1] = count[i] + count_in[i]
                count_move(i + 1).start()

        kept = 1 - (s + 12) // 16
        slot = kept * (SLOTS + s) + (1 - kept) * lax.rem(s + 8, SLOTS)
        for e in range(2):
            adj_copy(gather_place(s, e), slot, e).wait()
        right = jnp.concatenate([piece(feats_all, s, e)[...] for e in range(2)], axis=0)
        for m in range(0, rows, M_CHUNK):
            at = pl.ds(m, M_CHUNK)
            acc_one[at, :] += _dot(adj_buf[slot, at, :], right)
        fetch(s - 4 + SLOTS)

        @pl.when(s == 0)
        def _():
            for e in range(2):
                kept_copy(3, e).start()

        @pl.when((s >= 1) & (s < 1 + SLOTS))
        def _():
            for e in range(2):
                slab_copy(s - 1, e).start()

        return carry

    lax.fori_loop(0, 16, step_one, 0)

    aggs_all[me] = acc_one[...].astype(BF16)
    send_own(1, aggs_all)

    def hidden_step(s, dst):
        for e in range(2):
            pre = _dot(piece(aggs_all, s, e)[...], w_one_b[...])
            dst[pl.ds(e * quarter, quarter), :] = jnp.maximum(pre, 0.0).astype(BF16)

    def step_two(s, now, then):
        if then is not None:
            gather_step(1, aggs_all, s + 1)

        kept = 1 - (s + 12) // 16
        slot = kept * (SLOTS + s) + (1 - kept) * lax.rem(s + 8, SLOTS)

        @pl.when(s >= 4)
        def _():
            for e in range(2):
                adj_copy(gather_place(s, e), slot, e).wait()

        if then is not None:
            hidden_step(s + 1, then)
        right = now[...]
        for m in range(0, rows, M_TWO):
            at = pl.ds(m, M_TWO)
            acc_two[at, :] += _dot(adj_buf[slot, at, :], right)

        @pl.when(s >= 4)
        def _():
            fetch(s + 8 + SLOTS)

    def two_steps(i, carry):
        step_two(2 * i, hid, hid_next)
        step_two(2 * i + 1, hid_next, hid)
        return carry

    gather_step(1, aggs_all, jnp.int32(0))
    hidden_step(jnp.int32(0), hid)
    lax.fori_loop(0, 7, two_steps, 0)
    step_two(jnp.int32(14), hid, hid_next)
    step_two(jnp.int32(15), hid_next, None)

    count_move(2).wait_recv()
    total = (count[2] + count_in[2])[0:1, 0:1]
    agg_two[...] = acc_two[...].astype(BF16)
    logits = _dot_nt(w_two_t[0:48, :], agg_two[...])[:classes, :]
    weight = mask_v[...].astype(F32)
    shifted = logits - jnp.max(logits, axis=0, keepdims=True)
    log_prob = shifted - jnp.log(jnp.sum(jnp.exp(shifted), axis=0, keepdims=True))
    onehot = (lax.broadcasted_iota(jnp.int32, (classes, rows), 0) == lab_v[...]).astype(F32)
    picked = jnp.sum(onehot * log_prob, axis=0, keepdims=True)
    loss_sum = -jnp.sum(weight * picked)
    grad_t[:classes, :] = (weight * (jnp.exp(log_prob) - onehot) / total).astype(BF16)
    back_t[...] = _dot(w_two_b[...], grad_t[...]).astype(BF16)

    def pair_move(u):
        at = lax.rem(u, 4)
        return remote(stage.at[at], from_pair.at[at], pair_send.at[at], pair_recv.at[u], pair)

    def chip_move(u):
        link = lax.rem(u, 2)
        dev = me + (1 - link) * to_x + link * to_y
        return remote(to_chip.at[u], from_chip.at[link, u // 2], chip_send.at[u], chip_recv.at[link, u // 2], dev)

    def finish(u):
        pair_move(u).wait_recv()
        both = own_part[lax.rem(u, 2)] + from_pair[lax.rem(u, 4)]

        @pl.when(u < 12)
        def _():
            to_chip[u] = both.astype(BF16)
            chip_move(u).start()
            pl.semaphore_signal(pair_free, inc=1, device_id=(pair,), device_id_type=MESH)

        @pl.when(u >= 12)
        def _():
            own_sums[u - 12] = both

    def make_part(u, which):
        r = u + 24
        ring = 1 - u // 12
        kept = (1 - ring) * (u - 12)
        slot = ring * lax.rem(r, SLOTS) + (1 - ring) * (SLOTS + 2 * (1 - which) + kept // 2)
        col = pl.multiple_of((ring * which + lax.rem(kept, 2)) * quarter, quarter)

        @pl.when(u < 12)
        def _():
            part_copy(r, which).wait()

        part = _dot(back_t[...], adj_buf[slot, :, pl.ds(col, quarter)])
        if which == 0:
            stage[lax.rem(u, 4)] = part
            pair_move(u).start()
        else:
            own_part[lax.rem(u, 2)] = part
            fetch(r + SLOTS)

    def step_three(u, carry):
        @pl.when(u >= 4)
        def _():
            pair_move(u).wait_send()
            pl.semaphore_wait(pair_free, 1)

        make_part(u, 0)

        @pl.when(u >= 3)
        def _():
            finish(u - 1)

        make_part(u, 1)
        return carry

    first, second = jnp.int32(0), jnp.int32(1)
    make_part(first, 0)
    make_part(second, 0)
    make_part(first, 1)
    finish(first)
    make_part(second, 1)
    finish(second)
    lax.fori_loop(2, 16, step_three, 0)
    finish(jnp.int32(15))
    for u in range(12, 16):
        pair_move(u).wait_send()

    part_two = _dot(grad_t[0:48, :], agg_two[...])
    small[0, 0:40, :] = part_two[0:classes, 0:128]
    small[0, 40:80, :] = part_two[0:classes, 128:256]
    small[0, 80:96, :] = jnp.full((16, 128), loss_sum, F32)

    share = pl.ds(pl.multiple_of(core * 48, 8), 48)
    others = pl.ds(pl.multiple_of((1 - core) * 48, 8), 48)

    def small_move(i):
        at = pl.ds(0, 96) if i == 0 else share
        return remote(small.at[i, at], small_in.at[i, at], small_send.at[i], small_recv.at[i],
                      (pair, x_next, y_next)[i])

    small_move(0).start()
    pre_t[...] = _dot_nt(w_one_t[...], aggs_all[me])

    small_move(0).wait_recv()
    small[1] = small[0] + small_in[0]
    small_move(1).start()

    relays = []
    for k in range(2):
        for link in range(2):
            chip_move(2 * k + link).wait_recv()
            move = remote(from_chip.at[link, k], from_chip.at[1 - link, 6 + k], relay_send.at[link, k],
                          chip_recv.at[1 - link, 6 + k], (y_next, x_next)[link])
            move.start()
            relays.append(move)

    for j in range(4):
        for link in range(2):
            chip_move(4 + 2 * j + link).wait_recv()
            own_sums[j] += from_chip[link, 2 + j].astype(F32)
    small_move(1).wait_recv()
    small[2, share, :] = small[1, share, :] + small_in[1, share, :]
    small_move(2).start()
    red_one = jnp.zeros((256, 128), F32)
    for k in range(2):
        for link in range(2):
            j = 2 * (1 - link) + k
            relays[2 * k + 1 - link].wait_recv()
            d_hidden = own_sums[j] + from_chip[link, 6 + k].astype(F32)
            keep = pre_t[:, pl.ds(j * quarter, quarter)] > 0.0
            grad_one = jnp.where(keep, d_hidden, 0.0).astype(BF16)
            red_one += _dot(grad_one, aggs_all[me, pl.ds(j * quarter, quarter), :])
    red[...] = red_one

    n_half = red.shape[0] // 2
    n_part = n_half // 2
    mine = pl.multiple_of(core * n_half, 8)
    other = pl.multiple_of((1 - core) * n_half, 8)

    move = remote(red.at[pl.ds(other, n_half)], red_pair, red_send.at[0], red_recv.at[0], pair)
    move.start()
    move.wait_recv()
    red_link[...] = red[pl.ds(mine, n_half), :] + red_pair[...]
    moves = [
        remote(red_link.at[pl.ds(i * n_part, n_part)], red_next.at[pl.ds(i * n_part, n_part)],
               red_send.at[1 + i], red_recv.at[1 + i], (x_next, y_next)[i])
        for i in range(2)
    ]
    for m in moves:
        m.start()
    for m in moves:
        m.wait_recv()
    red_pair2 = red_link[...] + red_next[...]
    red_last[0] = red_pair2
    lasts = [
        remote(red_last.at[0, pl.ds(i * n_part, n_part)], red_last.at[1, pl.ds(i * n_part, n_part)],
               red_send.at[3 + i], red_recv.at[3 + i], (y_next, x_next)[i])
        for i in range(2)
    ]
    for m in lasts:
        m.start()
    for m in lasts:
        m.wait_recv()
    red_out[pl.ds(mine, n_half), :] = red_last[0] + red_last[1]
    ref = red_out.at[pl.ds(mine, n_half)]
    back = remote(ref, ref, red_send.at[5], red_recv.at[5], pair)
    back.start()
    small_move(2).wait_recv()
    small[3, share, :] = small[2, share, :] + small_in[2, share, :]
    small_back = remote(small.at[3, share], small.at[3, share], small_send.at[3], small_recv.at[3], pair)
    small_back.start()
    remote(small.at[3, others], small.at[3, others], small_send.at[3], small_recv.at[3], pair).wait_recv()
    ref_in = red_out.at[pl.ds(other, n_half)]
    remote(ref_in, ref_in, red_send.at[5], red_recv.at[5], pair).wait_recv()

    out[0:256, :] = red_out[...]
    out[256:336, :] = small[3, 0:80, :]
    out[336:352, :] = small[3, 80:96, :] / total

    move.wait_send()
    for m in moves + lasts + [back, small_back]:
        m.wait_send()
    for i in range(3):
        count_move(i).wait_send()
        small_move(i).wait_send()
    for ph, buf in ((0, feats_all), (1, aggs_all)):
        for to in range(2, 16):
            for e in range(2):
                send_piece(ph, buf, to, e, to, pair).wait_send()
    for u in range(12):
        chip_move(u).wait_send()
    for relay in relays:
        relay.wait_send()


def _finish(sums, out_loss, out_one, out_two):
    classes = out_two.shape[0]
    out_one[...] = sums[0:256, :].T
    out_two[:, 0:128] = sums[256:256 + classes, :]
    out_two[:, 128:256] = sums[256 + classes:256 + 2 * classes, :]
    out_loss[...] = sums[336:337, 0:1]


def solution(mesh):
    def step(adj, feat, w_one, w_two, labels, mask):
        rows, nodes = adj.shape
        feat_dim, hidden = w_one.shape
        classes = w_two.shape[1]
        parts = nodes // rows
        any_spec = pl.BlockSpec(memory_space=pltpu.HBM)
        vmem = pl.BlockSpec(memory_space=pltpu.VMEM)
        quarter = rows // 4
        scratch = [
            pltpu.VMEM((parts, rows, feat_dim), BF16),
            pltpu.VMEM((parts, rows, feat_dim), BF16),
            pltpu.VMEM((rows // 2, hidden), BF16),
            pltpu.VMEM((rows // 2, hidden), BF16),
            pltpu.VMEM((rows, feat_dim), F32),
            pltpu.VMEM((rows, hidden), F32),
            pltpu.VMEM((rows, hidden), BF16),
            pltpu.VMEM((hidden, rows), BF16),
            pltpu.VMEM((128, rows), BF16),
            pltpu.VMEM((hidden, rows), F32),
            pltpu.VMEM((2, hidden, quarter), F32),
            pltpu.VMEM((4, hidden, quarter), F32),
            pltpu.VMEM((4, hidden, quarter), F32),
            pltpu.VMEM((4, hidden, quarter), F32),
            pltpu.VMEM((12, hidden, quarter), BF16),
            pltpu.VMEM((2, 8, hidden, quarter), BF16),
            pltpu.VMEM((SLOTS + 4, rows, rows // 2), BF16),
            pltpu.VMEM((feat_dim, hidden), F32),
            pltpu.VMEM((classes, hidden), F32),
            pltpu.VMEM((feat_dim, hidden), BF16),
            pltpu.VMEM((hidden, feat_dim), BF16),
            pltpu.VMEM((hidden, 128), BF16),
            pltpu.VMEM((128, hidden), BF16),
            pltpu.VMEM((1, rows), jnp.int32),
            pltpu.VMEM((1, rows), jnp.int32),
            pltpu.VMEM((3, 8, 128), F32),
            pltpu.VMEM((3, 8, 128), F32),
            pltpu.VMEM((256, 128), F32),
            pltpu.VMEM((128, 128), F32),
            pltpu.VMEM((128, 128), F32),
            pltpu.VMEM((128, 128), F32),
            pltpu.VMEM((2, 128, 128), F32),
            pltpu.VMEM((256, 128), F32),
            pltpu.VMEM((4, 96, 128), F32),
            pltpu.VMEM((3, 96, 128), F32),
            pltpu.SemaphoreType.DMA((SLOTS + 4, 2)),
            pltpu.SemaphoreType.DMA((5,)),
            pltpu.SemaphoreType.DMA((2, 32)),
            pltpu.SemaphoreType.DMA((2, 32)),
            pltpu.SemaphoreType.DMA((3,)),
            pltpu.SemaphoreType.DMA((3,)),
            pltpu.SemaphoreType.DMA((4,)),
            pltpu.SemaphoreType.DMA((16,)),
            pltpu.SemaphoreType.REGULAR,
            pltpu.SemaphoreType.DMA((12,)),
            pltpu.SemaphoreType.DMA((2, 8)),
            pltpu.SemaphoreType.DMA((6,)),
            pltpu.SemaphoreType.DMA((6,)),
            pltpu.SemaphoreType.DMA((4,)),
            pltpu.SemaphoreType.DMA((4,)),
            pltpu.SemaphoreType.DMA((2, 2)),
        ]
        sums = pl.pallas_call(
            _kernel,
            out_shape=jax.ShapeDtypeStruct((352, 128), F32),
            in_specs=[any_spec] * 6,
            out_specs=vmem,
            scratch_shapes=scratch,
            compiler_params=pltpu.CompilerParams(
                collective_id=0, has_side_effects=True, vmem_limit_bytes=67_000_000),
            name="gcn_step",
        )(adj, feat, w_one, w_two.T, labels.reshape(1, rows), mask.reshape(1, rows))
        loss, dw_one, dw_two_t = pl.pallas_call(
            _finish,
            out_shape=(
                jax.ShapeDtypeStruct((1, 1), F32),
                jax.ShapeDtypeStruct((feat_dim, hidden), F32),
                jax.ShapeDtypeStruct((classes, hidden), F32),
            ),
            in_specs=[vmem],
            out_specs=(vmem, vmem, vmem),
            name="gcn_finish",
        )(sums)
        return loss.reshape(1), dw_one, dw_two_t.T

    return jax.shard_map(
        step,
        mesh=mesh,
        in_specs=(P(AXIS, None), P(AXIS, None), P(None, None), P(None, None), P(AXIS), P(AXIS)),
        out_specs=(P(None), P(None, None), P(None, None)),
        check_vma=False,
    )
```

```python
import jax
import jax.numpy as jnp
from jax import lax
from jax.experimental import pallas as pl
from jax.experimental.pallas import tpu as pltpu
from jax.sharding import PartitionSpec as P

AXIS = "nodes"
MESH = pl.DeviceIdType.MESH
F32 = jnp.float32
BF16 = jnp.bfloat16

SLOTS = 3
M_CHUNK = 256
M_TWO = 512


def _dot(a, b):
    return jnp.dot(a, b, preferred_element_type=F32)


def _dot_nt(a, b):
    return lax.dot_general(a, b, (((1,), (1,)), ((), ())), preferred_element_type=F32)


def _kernel(
    adj, feat, w_one, w_two, labels, mask,
    out,
    feats_all, aggs_all, hid, hid_next, acc_one, acc_two, agg_two, back_t, grad_t, pre_t,
    own_part, own_sums, stage, from_pair, to_chip, from_chip, adj_buf,
    w_one_f, w_two_f, w_one_b, w_one_t, w_two_b, w_two_t, lab_v, mask_v, count, count_in,
    red, red_pair, red_link, red_next, red_last, red_out, small, small_in,
    adj_sem, load_sem, gather_send, gather_recv, count_send, count_recv,
    pair_send, pair_recv, pair_free, chip_send, chip_recv, red_send, red_recv, small_send, small_recv, relay_send,
):
    rows = feat.shape[0]
    quarter = rows // 4
    classes = w_two.shape[0]
    me = lax.axis_index(AXIS)
    core, chip_x, chip_y = lax.rem(me, 2), lax.rem(me // 2, 2), me // 4
    to_pair, to_x, to_y = 1 - 2 * core, 2 - 4 * chip_x, 4 - 8 * chip_y
    pair, x_next, y_next = me + to_pair, me + to_x, me + to_y

    def remote(src, dst, send, recv, dev):
        return pltpu.make_async_remote_copy(
            src_ref=src, dst_ref=dst, send_sem=send, recv_sem=recv, device_id=(dev,), device_id_type=MESH)

    def gather_place(s, e):
        low = 1 - (s + 12) // 16
        far = s // 12
        near = 1 - low - far
        flip = low * (s // 2) + (1 - low) * lax.rem(s, 2)
        blk = me + flip * to_pair + (near * (1 - e) + far) * to_x + (near * e + far) * to_y
        part = (low * (2 * lax.rem(s, 2) + e) + near * lax.rem(s // 2 + 2 + 2 * e, 4) + far * (s // 2 - 6 + 2 * e))
        return blk, part

    def reduce_place(u):
        own = u // 12
        diag = 1 - (u + 12) // 16
        near = 1 - own - diag
        link = lax.rem(u, 2)
        nx = diag + near * (1 - link)
        ny = diag + near * link
        part = own * (u - 12) + diag * (2 * link + u // 2) + near * (u // 2 - 2)
        return me + nx * to_x + ny * to_y, part

    def adj_copy(place, slot, e):
        blk, part = place
        col = pl.multiple_of(blk * rows + part * quarter, quarter)
        return pltpu.make_async_copy(
            adj.at[:, pl.ds(col, quarter)], adj_buf.at[slot, :, pl.ds(e * quarter, quarter)], adj_sem.at[slot, e])

    def kept_copy(s, e):
        return adj_copy(gather_place(s, e), SLOTS + s, e)

    def slab_copy(r, e):
        return adj_copy(gather_place(lax.rem(r, 12) + 4, e), lax.rem(r, SLOTS), e)

    def part_copy(r, e):
        blk, part = reduce_place(r - 24)
        return adj_copy((blk + to_pair * (1 - e), part), lax.rem(r, SLOTS), e)

    def fetch(r):
        @pl.when((r >= SLOTS) & (r < 24))
        def _():
            for e in range(2):
                slab_copy(r, e).start()

        @pl.when((r >= 24) & (r < 36))
        def _():
            for e in range(2):
                part_copy(r, e).start()

    loads = [
        pltpu.make_async_copy(feat, feats_all.at[me], load_sem.at[0]),
        pltpu.make_async_copy(mask, mask_v, load_sem.at[1]),
        pltpu.make_async_copy(w_one, w_one_f, load_sem.at[2]),
        pltpu.make_async_copy(w_two, w_two_f, load_sem.at[3]),
        pltpu.make_async_copy(labels, lab_v, load_sem.at[4]),
    ]
    for load in loads:
        load.start()
    for e in range(2):
        kept_copy(0, e).start()

    barrier = pltpu.get_barrier_semaphore()
    for dev in (pair, x_next, y_next):
        pl.semaphore_signal(barrier, inc=1, device_id=(dev,), device_id_type=MESH)
    acc_one[...] = jnp.zeros_like(acc_one)
    acc_two[...] = jnp.zeros_like(acc_two)
    grad_t[...] = jnp.zeros_like(grad_t)
    pl.semaphore_wait(barrier, 3)

    def piece(buf, s, e):
        blk, part = gather_place(s, e)
        return buf.at[blk, pl.ds(pl.multiple_of(part * quarter, quarter), quarter), :]

    def send_piece(ph, buf, s, e, to, dev):
        ref = piece(buf, s, e)
        at = 2 * to + e
        return remote(ref, ref, gather_send.at[ph, at], gather_recv.at[ph, at], dev)

    def send_own(ph, buf):
        for i in range(4):
            for e, dev in ((0, x_next), (1, y_next)):
                part = (i + 2 * e) % 4
                ref = buf.at[me, pl.ds(part * quarter, quarter), :]
                at = 2 * (4 + 2 * i) + e
                remote(ref, ref, gather_send.at[ph, at], gather_recv.at[ph, at], dev).start()

    def gather_step(ph, buf, s):
        for e in range(2):
            @pl.when(s >= 2)
            def _():
                send_piece(ph, buf, s, e, s, pair).wait_recv()

            @pl.when((s == 4) | (s == 6))
            def _():
                send_piece(ph, buf, s, e, s + 8, (y_next, x_next)[e]).start()

            @pl.when(s < 2)
            def _():
                send_piece(ph, buf, s, e, s + 2, pair).start()

            @pl.when((s >= 4) & (lax.rem(s, 2) == 0))
            def _():
                send_piece(ph, buf, s, e, s + 1, pair).start()

    def count_move(i):
        return remote(count.at[i], count_in.at[i], count_send.at[i], count_recv.at[i], (pair, x_next, y_next)[i])

    loads[0].wait()
    send_own(0, feats_all)
    for e in range(2):
        kept_copy(1, e).start()
        kept_copy(2, e).start()
    for load in loads[1:]:
        load.wait()
    count[0] = jnp.full((8, 128), jnp.sum(mask_v[...].astype(F32)), F32)
    count_move(0).start()
    w_one_b[...] = w_one_f[...].astype(BF16)
    w_one_t[...] = w_one_f[...].T.astype(BF16)
    w_two_t[...] = jnp.zeros_like(w_two_t)
    w_two_t[:classes, :] = w_two_f[...].astype(BF16)
    w_two_b[...] = w_two_t[...].astype(F32).T.astype(BF16)

    def step_one(s, carry):
        gather_step(0, feats_all, s)

        for i, when in enumerate((1, 12)):
            @pl.when(s == when)
            def _(i=i):
                count_move(i).wait_recv()
                count[i + 1] = count[i] + count_in[i]
                count_move(i + 1).start()

        kept = 1 - (s + 12) // 16
        slot = kept * (SLOTS + s) + (1 - kept) * lax.rem(s + 8, SLOTS)
        for e in range(2):
            adj_copy(gather_place(s, e), slot, e).wait()
        right = jnp.concatenate([piece(feats_all, s, e)[...] for e in range(2)], axis=0)
        for m in range(0, rows, M_CHUNK):
            at = pl.ds(m, M_CHUNK)
            acc_one[at, :] += _dot(adj_buf[slot, at, :], right)
        fetch(s - 4 + SLOTS)

        @pl.when(s == 0)
        def _():
            for e in range(2):
                kept_copy(3, e).start()

        @pl.when((s >= 1) & (s < 1 + SLOTS))
        def _():
            for e in range(2):
                slab_copy(s - 1, e).start()

        return carry

    lax.fori_loop(0, 16, step_one, 0)

    aggs_all[me] = acc_one[...].astype(BF16)
    send_own(1, aggs_all)

    def hidden_step(s, dst):
        for e in range(2):
            pre = _dot(piece(aggs_all, s, e)[...], w_one_b[...])
            dst[pl.ds(e * quarter, quarter), :] = jnp.maximum(pre, 0.0).astype(BF16)

    def step_two(s, now, then):
        if then is not None:
            gather_step(1, aggs_all, s + 1)

        kept = 1 - (s + 12) // 16
        slot = kept * (SLOTS + s) + (1 - kept) * lax.rem(s + 8, SLOTS)

        @pl.when(s >= 4)
        def _():
            for e in range(2):
                adj_copy(gather_place(s, e), slot, e).wait()

        if then is not None:
            hidden_step(s + 1, then)
        right = now[...]
        for m in range(0, rows, M_TWO):
            at = pl.ds(m, M_TWO)
            acc_two[at, :] += _dot(adj_buf[slot, at, :], right)

        @pl.when(s >= 4)
        def _():
            fetch(s + 8 + SLOTS)

    def two_steps(i, carry):
        step_two(2 * i, hid, hid_next)
        step_two(2 * i + 1, hid_next, hid)
        return carry

    gather_step(1, aggs_all, jnp.int32(0))
    hidden_step(jnp.int32(0), hid)
    lax.fori_loop(0, 7, two_steps, 0)
    step_two(jnp.int32(14), hid, hid_next)
    step_two(jnp.int32(15), hid_next, None)

    count_move(2).wait_recv()
    total = (count[2] + count_in[2])[0:1, 0:1]
    agg_two[...] = acc_two[...].astype(BF16)
    logits = _dot_nt(w_two_t[0:48, :], agg_two[...])[:classes, :]
    weight = mask_v[...].astype(F32)
    shifted = logits - jnp.max(logits, axis=0, keepdims=True)
    log_prob = shifted - jnp.log(jnp.sum(jnp.exp(shifted), axis=0, keepdims=True))
    onehot = (lax.broadcasted_iota(jnp.int32, (classes, rows), 0) == lab_v[...]).astype(F32)
    picked = jnp.sum(onehot * log_prob, axis=0, keepdims=True)
    loss_sum = -jnp.sum(weight * picked)
    grad_t[:classes, :] = (weight * (jnp.exp(log_prob) - onehot) / total).astype(BF16)
    back_t[...] = _dot(w_two_b[...], grad_t[...]).astype(BF16)

    def pair_move(u):
        at = lax.rem(u, 4)
        return remote(stage.at[at], from_pair.at[at], pair_send.at[at], pair_recv.at[u], pair)

    def chip_move(u):
        link = lax.rem(u, 2)
        dev = me + (1 - link) * to_x + link * to_y
        return remote(to_chip.at[u], from_chip.at[link, u // 2], chip_send.at[u], chip_recv.at[link, u // 2], dev)

    def finish(u):
        pair_move(u).wait_recv()
        both = own_part[lax.rem(u, 2)] + from_pair[lax.rem(u, 4)]

        @pl.when(u < 12)
        def _():
            to_chip[u] = both.astype(BF16)
            chip_move(u).start()
            pl.semaphore_signal(pair_free, inc=1, device_id=(pair,), device_id_type=MESH)

        @pl.when(u >= 12)
        def _():
            own_sums[u - 12] = both

    def make_part(u, which):
        r = u + 24
        ring = 1 - u // 12
        kept = (1 - ring) * (u - 12)
        slot = ring * lax.rem(r, SLOTS) + (1 - ring) * (SLOTS + 2 * (1 - which) + kept // 2)
        col = pl.multiple_of((ring * which + lax.rem(kept, 2)) * quarter, quarter)

        @pl.when(u < 12)
        def _():
            part_copy(r, which).wait()

        part = _dot(back_t[...], adj_buf[slot, :, pl.ds(col, quarter)])
        if which == 0:
            stage[lax.rem(u, 4)] = part
            pair_move(u).start()
        else:
            own_part[lax.rem(u, 2)] = part
            fetch(r + SLOTS)

    def step_three(u, carry):
        @pl.when(u >= 4)
        def _():
            pair_move(u).wait_send()
            pl.semaphore_wait(pair_free, 1)

        make_part(u, 0)

        @pl.when(u >= 3)
        def _():
            finish(u - 1)

        make_part(u, 1)
        return carry

    first, second = jnp.int32(0), jnp.int32(1)
    make_part(first, 0)
    make_part(second, 0)
    make_part(first, 1)
    finish(first)
    make_part(second, 1)
    finish(second)
    lax.fori_loop(2, 16, step_three, 0)
    finish(jnp.int32(15))
    for u in range(12, 16):
        pair_move(u).wait_send()

    part_two = _dot(grad_t[0:48, :], agg_two[...])
    small[0, 0:40, :] = part_two[0:classes, 0:128]
    small[0, 40:80, :] = part_two[0:classes, 128:256]
    small[0, 80:96, :] = jnp.full((16, 128), loss_sum, F32)

    share = pl.ds(pl.multiple_of(core * 48, 8), 48)
    others = pl.ds(pl.multiple_of((1 - core) * 48, 8), 48)

    def small_move(i):
        at = pl.ds(0, 96) if i == 0 else share
        return remote(small.at[i, at], small_in.at[i, at], small_send.at[i], small_recv.at[i],
                      (pair, x_next, y_next)[i])

    small_move(0).start()
    pre_t[...] = _dot_nt(w_one_t[...], aggs_all[me])

    small_move(0).wait_recv()
    small[1] = small[0] + small_in[0]

    relays = []
    for k in range(2):
        for link in range(2):
            chip_move(2 * k + link).wait_recv()
            move = remote(from_chip.at[link, k], from_chip.at[1 - link, 6 + k], relay_send.at[link, k],
                          chip_recv.at[1 - link, 6 + k], (y_next, x_next)[link])
            move.start()
            relays.append(move)
    small_move(1).start()

    for j in range(4):
        for link in range(2):
            chip_move(4 + 2 * j + link).wait_recv()
            own_sums[j] += from_chip[link, 2 + j].astype(F32)
    red_one = jnp.zeros((256, 128), F32)
    for k in range(2):
        for link in range(2):
            j = 2 * (1 - link) + k
            relays[2 * k + 1 - link].wait_recv()
            d_hidden = own_sums[j] + from_chip[link, 6 + k].astype(F32)
            keep = pre_t[:, pl.ds(j * quarter, quarter)] > 0.0
            grad_one = jnp.where(keep, d_hidden, 0.0).astype(BF16)
            red_one += _dot(grad_one, aggs_all[me, pl.ds(j * quarter, quarter), :])
    red[...] = red_one

    n_half = red.shape[0] // 2
    n_part = n_half // 2
    mine = pl.multiple_of(core * n_half, 8)
    other = pl.multiple_of((1 - core) * n_half, 8)

    move = remote(red.at[pl.ds(other, n_half)], red_pair, red_send.at[0], red_recv.at[0], pair)
    move.start()
    small_move(1).wait_recv()
    small[2, share, :] = small[1, share, :] + small_in[1, share, :]
    small_move(2).start()
    move.wait_recv()
    red_link[...] = red[pl.ds(mine, n_half), :] + red_pair[...]
    moves = [
        remote(red_link.at[pl.ds(i * n_part, n_part)], red_next.at[pl.ds(i * n_part, n_part)],
               red_send.at[1 + i], red_recv.at[1 + i], (x_next, y_next)[i])
        for i in range(2)
    ]
    for m in moves:
        m.start()
    for m in moves:
        m.wait_recv()
    red_pair2 = red_link[...] + red_next[...]
    red_last[0] = red_pair2
    lasts = [
        remote(red_last.at[0, pl.ds(i * n_part, n_part)], red_last.at[1, pl.ds(i * n_part, n_part)],
               red_send.at[3 + i], red_recv.at[3 + i], (y_next, x_next)[i])
        for i in range(2)
    ]
    for m in lasts:
        m.start()
    for m in lasts:
        m.wait_recv()
    red_out[pl.ds(mine, n_half), :] = red_last[0] + red_last[1]
    ref = red_out.at[pl.ds(mine, n_half)]
    back = remote(ref, ref, red_send.at[5], red_recv.at[5], pair)
    back.start()
    small_move(2).wait_recv()
    small[3, share, :] = small[2, share, :] + small_in[2, share, :]
    small_back = remote(small.at[3, share], small.at[3, share], small_send.at[3], small_recv.at[3], pair)
    small_back.start()
    remote(small.at[3, others], small.at[3, others], small_send.at[3], small_recv.at[3], pair).wait_recv()
    ref_in = red_out.at[pl.ds(other, n_half)]
    remote(ref_in, ref_in, red_send.at[5], red_recv.at[5], pair).wait_recv()

    out[0:256, :] = red_out[...]
    out[256:336, :] = small[3, 0:80, :]
    out[336:352, :] = small[3, 80:96, :] / total

    move.wait_send()
    for m in moves + lasts + [back, small_back]:
        m.wait_send()
    for i in range(3):
        count_move(i).wait_send()
        small_move(i).wait_send()
    for ph, buf in ((0, feats_all), (1, aggs_all)):
        for to in range(2, 16):
            for e in range(2):
                send_piece(ph, buf, to, e, to, pair).wait_send()
    for u in range(12):
        chip_move(u).wait_send()
    for relay in relays:
        relay.wait_send()


def _finish(sums, out_loss, out_one, out_two):
    classes = out_two.shape[0]
    out_one[...] = sums[0:256, :].T
    out_two[:, 0:128] = sums[256:256 + classes, :]
    out_two[:, 128:256] = sums[256 + classes:256 + 2 * classes, :]
    out_loss[...] = sums[336:337, 0:1]


def solution(mesh):
    def step(adj, feat, w_one, w_two, labels, mask):
        rows, nodes = adj.shape
        feat_dim, hidden = w_one.shape
        classes = w_two.shape[1]
        parts = nodes // rows
        any_spec = pl.BlockSpec(memory_space=pltpu.HBM)
        vmem = pl.BlockSpec(memory_space=pltpu.VMEM)
        quarter = rows // 4
        scratch = [
            pltpu.VMEM((parts, rows, feat_dim), BF16),
            pltpu.VMEM((parts, rows, feat_dim), BF16),
            pltpu.VMEM((rows // 2, hidden), BF16),
            pltpu.VMEM((rows // 2, hidden), BF16),
            pltpu.VMEM((rows, feat_dim), F32),
            pltpu.VMEM((rows, hidden), F32),
            pltpu.VMEM((rows, hidden), BF16),
            pltpu.VMEM((hidden, rows), BF16),
            pltpu.VMEM((128, rows), BF16),
            pltpu.VMEM((hidden, rows), F32),
            pltpu.VMEM((2, hidden, quarter), F32),
            pltpu.VMEM((4, hidden, quarter), F32),
            pltpu.VMEM((4, hidden, quarter), F32),
            pltpu.VMEM((4, hidden, quarter), F32),
            pltpu.VMEM((12, hidden, quarter), BF16),
            pltpu.VMEM((2, 8, hidden, quarter), BF16),
            pltpu.VMEM((SLOTS + 4, rows, rows // 2), BF16),
            pltpu.VMEM((feat_dim, hidden), F32),
            pltpu.VMEM((classes, hidden), F32),
            pltpu.VMEM((feat_dim, hidden), BF16),
            pltpu.VMEM((hidden, feat_dim), BF16),
            pltpu.VMEM((hidden, 128), BF16),
            pltpu.VMEM((128, hidden), BF16),
            pltpu.VMEM((1, rows), jnp.int32),
            pltpu.VMEM((1, rows), jnp.int32),
            pltpu.VMEM((3, 8, 128), F32),
            pltpu.VMEM((3, 8, 128), F32),
            pltpu.VMEM((256, 128), F32),
            pltpu.VMEM((128, 128), F32),
            pltpu.VMEM((128, 128), F32),
            pltpu.VMEM((128, 128), F32),
            pltpu.VMEM((2, 128, 128), F32),
            pltpu.VMEM((256, 128), F32),
            pltpu.VMEM((4, 96, 128), F32),
            pltpu.VMEM((3, 96, 128), F32),
            pltpu.SemaphoreType.DMA((SLOTS + 4, 2)),
            pltpu.SemaphoreType.DMA((5,)),
            pltpu.SemaphoreType.DMA((2, 32)),
            pltpu.SemaphoreType.DMA((2, 32)),
            pltpu.SemaphoreType.DMA((3,)),
            pltpu.SemaphoreType.DMA((3,)),
            pltpu.SemaphoreType.DMA((4,)),
            pltpu.SemaphoreType.DMA((16,)),
            pltpu.SemaphoreType.REGULAR,
            pltpu.SemaphoreType.DMA((12,)),
            pltpu.SemaphoreType.DMA((2, 8)),
            pltpu.SemaphoreType.DMA((6,)),
            pltpu.SemaphoreType.DMA((6,)),
            pltpu.SemaphoreType.DMA((4,)),
            pltpu.SemaphoreType.DMA((4,)),
            pltpu.SemaphoreType.DMA((2, 2)),
        ]
        sums = pl.pallas_call(
            _kernel,
            out_shape=jax.ShapeDtypeStruct((352, 128), F32),
            in_specs=[any_spec] * 6,
            out_specs=vmem,
            scratch_shapes=scratch,
            compiler_params=pltpu.CompilerParams(
                collective_id=0, has_side_effects=True, vmem_limit_bytes=67_000_000),
            name="gcn_step",
        )(adj, feat, w_one, w_two.T, labels.reshape(1, rows), mask.reshape(1, rows))
        loss, dw_one, dw_two_t = pl.pallas_call(
            _finish,
            out_shape=(
                jax.ShapeDtypeStruct((1, 1), F32),
                jax.ShapeDtypeStruct((feat_dim, hidden), F32),
                jax.ShapeDtypeStruct((classes, hidden), F32),
            ),
            in_specs=[vmem],
            out_specs=(vmem, vmem, vmem),
            name="gcn_finish",
        )(sums)
        return loss.reshape(1), dw_one, dw_two_t.T

    return jax.shard_map(
        step,
        mesh=mesh,
        in_specs=(P(AXIS, None), P(AXIS, None), P(None, None), P(None, None), P(AXIS), P(AXIS)),
        out_specs=(P(None), P(None, None), P(None, None)),
        check_vma=False,
    )
```

```python
import jax
import jax.numpy as jnp
from jax import lax
from jax.experimental import pallas as pl
from jax.experimental.pallas import tpu as pltpu
from jax.sharding import PartitionSpec as P

AXIS = "nodes"
MESH = pl.DeviceIdType.MESH
F32 = jnp.float32
BF16 = jnp.bfloat16

SLOTS = 3
M_CHUNK = 256
M_TWO = 512


def _dot(a, b):
    return jnp.dot(a, b, preferred_element_type=F32)


def _dot_nt(a, b):
    return lax.dot_general(a, b, (((1,), (1,)), ((), ())), preferred_element_type=F32)


def _kernel(
    adj, feat, w_one, w_two, labels, mask,
    out,
    feats_all, aggs_all, hid, hid_next, acc_one, acc_two, agg_two, back_t, grad_t, pre_t,
    own_part, own_sums, stage, from_pair, to_chip, from_chip, adj_buf,
    w_one_f, w_two_f, w_one_b, w_one_t, w_two_b, w_two_t, lab_v, mask_v, count, count_in,
    red, red_pair, red_link, red_next, red_last, red_out, small, small_in,
    adj_sem, load_sem, gather_send, gather_recv, count_send, count_recv,
    pair_send, pair_recv, pair_free, chip_send, chip_recv, red_send, red_recv, small_send, small_recv, relay_send,
):
    rows = feat.shape[0]
    quarter = rows // 4
    classes = w_two.shape[0]
    me = lax.axis_index(AXIS)
    core, chip_x, chip_y = lax.rem(me, 2), lax.rem(me // 2, 2), me // 4
    to_pair, to_x, to_y = 1 - 2 * core, 2 - 4 * chip_x, 4 - 8 * chip_y
    pair, x_next, y_next = me + to_pair, me + to_x, me + to_y

    def remote(src, dst, send, recv, dev):
        return pltpu.make_async_remote_copy(
            src_ref=src, dst_ref=dst, send_sem=send, recv_sem=recv, device_id=(dev,), device_id_type=MESH)

    def gather_place(s, e):
        low = 1 - (s + 12) // 16
        far = s // 12
        near = 1 - low - far
        flip = low * (s // 2) + (1 - low) * lax.rem(s, 2)
        blk = me + flip * to_pair + (near * (1 - e) + far) * to_x + (near * e + far) * to_y
        part = (low * (2 * lax.rem(s, 2) + e) + near * lax.rem(s // 2 + 2 + 2 * e, 4) + far * (s // 2 - 6 + 2 * e))
        return blk, part

    def reduce_place(u):
        own = u // 12
        diag = 1 - (u + 12) // 16
        near = 1 - own - diag
        link = lax.rem(u, 2)
        nx = diag + near * (1 - link)
        ny = diag + near * link
        part = own * (u - 12) + diag * (2 * link + u // 2) + near * (u // 2 - 2)
        return me + nx * to_x + ny * to_y, part

    def adj_copy(place, slot, e):
        blk, part = place
        col = pl.multiple_of(blk * rows + part * quarter, quarter)
        return pltpu.make_async_copy(
            adj.at[:, pl.ds(col, quarter)], adj_buf.at[slot, :, pl.ds(e * quarter, quarter)], adj_sem.at[slot, e])

    def kept_copy(s, e):
        return adj_copy(gather_place(s, e), SLOTS + s, e)

    def slab_copy(r, e):
        return adj_copy(gather_place(lax.rem(r, 12) + 4, e), lax.rem(r, SLOTS), e)

    def part_copy(r, e):
        blk, part = reduce_place(r - 24)
        return adj_copy((blk + to_pair * (1 - e), part), lax.rem(r, SLOTS), e)

    def fetch(r):
        @pl.when((r >= SLOTS) & (r < 24))
        def _():
            for e in range(2):
                slab_copy(r, e).start()

        @pl.when((r >= 24) & (r < 36))
        def _():
            for e in range(2):
                part_copy(r, e).start()

    loads = [
        pltpu.make_async_copy(feat, feats_all.at[me], load_sem.at[0]),
        pltpu.make_async_copy(mask, mask_v, load_sem.at[1]),
        pltpu.make_async_copy(w_one, w_one_f, load_sem.at[2]),
        pltpu.make_async_copy(w_two, w_two_f, load_sem.at[3]),
        pltpu.make_async_copy(labels, lab_v, load_sem.at[4]),
    ]
    for load in loads:
        load.start()
    for e in range(2):
        kept_copy(0, e).start()

    barrier = pltpu.get_barrier_semaphore()
    for dev in (pair, x_next, y_next):
        pl.semaphore_signal(barrier, inc=1, device_id=(dev,), device_id_type=MESH)
    acc_one[...] = jnp.zeros_like(acc_one)
    pl.semaphore_wait(barrier, 3)

    def piece(buf, s, e):
        blk, part = gather_place(s, e)
        return buf.at[blk, pl.ds(pl.multiple_of(part * quarter, quarter), quarter), :]

    def send_piece(ph, buf, s, e, to, dev):
        ref = piece(buf, s, e)
        at = 2 * to + e
        return remote(ref, ref, gather_send.at[ph, at], gather_recv.at[ph, at], dev)

    def send_own(ph, buf):
        for i in range(4):
            for e, dev in ((0, x_next), (1, y_next)):
                part = (i + 2 * e) % 4
                ref = buf.at[me, pl.ds(part * quarter, quarter), :]
                at = 2 * (4 + 2 * i) + e
                remote(ref, ref, gather_send.at[ph, at], gather_recv.at[ph, at], dev).start()

    def gather_step(ph, buf, s):
        for e in range(2):
            @pl.when(s >= 2)
            def _():
                send_piece(ph, buf, s, e, s, pair).wait_recv()

            @pl.when((s == 4) | (s == 6))
            def _():
                send_piece(ph, buf, s, e, s + 8, (y_next, x_next)[e]).start()

            @pl.when(s < 2)
            def _():
                send_piece(ph, buf, s, e, s + 2, pair).start()

            @pl.when((s >= 4) & (lax.rem(s, 2) == 0))
            def _():
                send_piece(ph, buf, s, e, s + 1, pair).start()

    def count_move(i):
        return remote(count.at[i], count_in.at[i], count_send.at[i], count_recv.at[i], (pair, x_next, y_next)[i])

    loads[0].wait()
    send_own(0, feats_all)
    for e in range(2):
        kept_copy(1, e).start()
        kept_copy(2, e).start()
    acc_two[...] = jnp.zeros_like(acc_two)
    grad_t[...] = jnp.zeros_like(grad_t)
    for load in loads[1:]:
        load.wait()
    count[0] = jnp.full((8, 128), jnp.sum(mask_v[...].astype(F32)), F32)
    count_move(0).start()
    w_one_b[...] = w_one_f[...].astype(BF16)
    w_one_t[...] = w_one_f[...].T.astype(BF16)
    w_two_t[...] = jnp.zeros_like(w_two_t)
    w_two_t[:classes, :] = w_two_f[...].astype(BF16)
    w_two_b[...] = w_two_t[...].astype(F32).T.astype(BF16)

    def step_one(s, carry):
        gather_step(0, feats_all, s)

        for i, when in enumerate((1, 12)):
            @pl.when(s == when)
            def _(i=i):
                count_move(i).wait_recv()
                count[i + 1] = count[i] + count_in[i]
                count_move(i + 1).start()

        kept = 1 - (s + 12) // 16
        slot = kept * (SLOTS + s) + (1 - kept) * lax.rem(s + 8, SLOTS)
        for e in range(2):
            adj_copy(gather_place(s, e), slot, e).wait()
        right = jnp.concatenate([piece(feats_all, s, e)[...] for e in range(2)], axis=0)
        for m in range(0, rows, M_CHUNK):
            at = pl.ds(m, M_CHUNK)
            acc_one[at, :] += _dot(adj_buf[slot, at, :], right)
        fetch(s - 4 + SLOTS)

        @pl.when(s == 0)
        def _():
            for e in range(2):
                kept_copy(3, e).start()

        @pl.when((s >= 1) & (s < 1 + SLOTS))
        def _():
            for e in range(2):
                slab_copy(s - 1, e).start()

        return carry

    lax.fori_loop(0, 16, step_one, 0)

    aggs_all[me] = acc_one[...].astype(BF16)
    send_own(1, aggs_all)

    def hidden_step(s, dst):
        for e in range(2):
            pre = _dot(piece(aggs_all, s, e)[...], w_one_b[...])
            dst[pl.ds(e * quarter, quarter), :] = jnp.maximum(pre, 0.0).astype(BF16)

    def step_two(s, now, then):
        if then is not None:
            gather_step(1, aggs_all, s + 1)

        kept = 1 - (s + 12) // 16
        slot = kept * (SLOTS + s) + (1 - kept) * lax.rem(s + 8, SLOTS)

        @pl.when(s >= 4)
        def _():
            for e in range(2):
                adj_copy(gather_place(s, e), slot, e).wait()

        if then is not None:
            hidden_step(s + 1, then)
        right = now[...]
        for m in range(0, rows, M_TWO):
            at = pl.ds(m, M_TWO)
            acc_two[at, :] += _dot(adj_buf[slot, at, :], right)

        @pl.when(s >= 4)
        def _():
            fetch(s + 8 + SLOTS)

    def two_steps(i, carry):
        step_two(2 * i, hid, hid_next)
        step_two(2 * i + 1, hid_next, hid)
        return carry

    gather_step(1, aggs_all, jnp.int32(0))
    hidden_step(jnp.int32(0), hid)
    lax.fori_loop(0, 7, two_steps, 0)
    step_two(jnp.int32(14), hid, hid_next)
    step_two(jnp.int32(15), hid_next, None)

    count_move(2).wait_recv()
    total = (count[2] + count_in[2])[0:1, 0:1]
    agg_two[...] = acc_two[...].astype(BF16)
    logits = _dot_nt(w_two_t[0:48, :], agg_two[...])[:classes, :]
    weight = mask_v[...].astype(F32)
    shifted = logits - jnp.max(logits, axis=0, keepdims=True)
    log_prob = shifted - jnp.log(jnp.sum(jnp.exp(shifted), axis=0, keepdims=True))
    onehot = (lax.broadcasted_iota(jnp.int32, (classes, rows), 0) == lab_v[...]).astype(F32)
    picked = jnp.sum(onehot * log_prob, axis=0, keepdims=True)
    loss_sum = -jnp.sum(weight * picked)
    grad_t[:classes, :] = (weight * (jnp.exp(log_prob) - onehot) / total).astype(BF16)
    back_t[...] = _dot(w_two_b[...], grad_t[...]).astype(BF16)

    def pair_move(u):
        at = lax.rem(u, 4)
        return remote(stage.at[at], from_pair.at[at], pair_send.at[at], pair_recv.at[u], pair)

    def chip_move(u):
        link = lax.rem(u, 2)
        dev = me + (1 - link) * to_x + link * to_y
        return remote(to_chip.at[u], from_chip.at[link, u // 2], chip_send.at[u], chip_recv.at[link, u // 2], dev)

    def finish(u):
        pair_move(u).wait_recv()
        both = own_part[lax.rem(u, 2)] + from_pair[lax.rem(u, 4)]

        @pl.when(u < 12)
        def _():
            to_chip[u] = both.astype(BF16)
            chip_move(u).start()
            pl.semaphore_signal(pair_free, inc=1, device_id=(pair,), device_id_type=MESH)

        @pl.when(u >= 12)
        def _():
            own_sums[u - 12] = both

    def make_part(u, which):
        r = u + 24
        ring = 1 - u // 12
        kept = (1 - ring) * (u - 12)
        slot = ring * lax.rem(r, SLOTS) + (1 - ring) * (SLOTS + 2 * (1 - which) + kept // 2)
        col = pl.multiple_of((ring * which + lax.rem(kept, 2)) * quarter, quarter)

        @pl.when(u < 12)
        def _():
            part_copy(r, which).wait()

        part = _dot(back_t[...], adj_buf[slot, :, pl.ds(col, quarter)])
        if which == 0:
            stage[lax.rem(u, 4)] = part
            pair_move(u).start()
        else:
            own_part[lax.rem(u, 2)] = part
            fetch(r + SLOTS)

    def step_three(u, carry):
        @pl.when(u >= 4)
        def _():
            pair_move(u).wait_send()
            pl.semaphore_wait(pair_free, 1)

        make_part(u, 0)

        @pl.when(u >= 3)
        def _():
            finish(u - 1)

        make_part(u, 1)
        return carry

    first, second = jnp.int32(0), jnp.int32(1)
    make_part(first, 0)
    make_part(second, 0)
    make_part(first, 1)
    finish(first)
    make_part(second, 1)
    finish(second)
    lax.fori_loop(2, 16, step_three, 0)
    finish(jnp.int32(15))
    for u in range(12, 16):
        pair_move(u).wait_send()

    part_two = _dot(grad_t[0:48, :], agg_two[...])
    small[0, 0:40, :] = part_two[0:classes, 0:128]
    small[0, 40:80, :] = part_two[0:classes, 128:256]
    small[0, 80:96, :] = jnp.full((16, 128), loss_sum, F32)

    share = pl.ds(pl.multiple_of(core * 48, 8), 48)
    others = pl.ds(pl.multiple_of((1 - core) * 48, 8), 48)

    def small_move(i):
        at = pl.ds(0, 96) if i == 0 else share
        return remote(small.at[i, at], small_in.at[i, at], small_send.at[i], small_recv.at[i],
                      (pair, x_next, y_next)[i])

    small_move(0).start()
    pre_t[...] = _dot_nt(w_one_t[...], aggs_all[me])

    small_move(0).wait_recv()
    small[1] = small[0] + small_in[0]

    relays = []
    for k in range(2):
        for link in range(2):
            chip_move(2 * k + link).wait_recv()
            move = remote(from_chip.at[link, k], from_chip.at[1 - link, 6 + k], relay_send.at[link, k],
                          chip_recv.at[1 - link, 6 + k], (y_next, x_next)[link])
            move.start()
            relays.append(move)
    small_move(1).start()

    for j in range(4):
        for link in range(2):
            chip_move(4 + 2 * j + link).wait_recv()
            own_sums[j] += from_chip[link, 2 + j].astype(F32)
    red_one = jnp.zeros((256, 128), F32)
    for k in range(2):
        for link in range(2):
            j = 2 * (1 - link) + k
            relays[2 * k + 1 - link].wait_recv()
            d_hidden = own_sums[j] + from_chip[link, 6 + k].astype(F32)
            keep = pre_t[:, pl.ds(j * quarter, quarter)] > 0.0
            grad_one = jnp.where(keep, d_hidden, 0.0).astype(BF16)
            red_one += _dot(grad_one, aggs_all[me, pl.ds(j * quarter, quarter), :])
    red[...] = red_one

    n_half = red.shape[0] // 2
    n_part = n_half // 2
    mine = pl.multiple_of(core * n_half, 8)
    other = pl.multiple_of((1 - core) * n_half, 8)

    move = remote(red.at[pl.ds(other, n_half)], red_pair, red_send.at[0], red_recv.at[0], pair)
    move.start()
    small_move(1).wait_recv()
    small[2, share, :] = small[1, share, :] + small_in[1, share, :]
    small_move(2).start()
    move.wait_recv()
    red_link[...] = red[pl.ds(mine, n_half), :] + red_pair[...]
    moves = [
        remote(red_link.at[pl.ds(i * n_part, n_part)], red_next.at[pl.ds(i * n_part, n_part)],
               red_send.at[1 + i], red_recv.at[1 + i], (x_next, y_next)[i])
        for i in range(2)
    ]
    for m in moves:
        m.start()
    for m in moves:
        m.wait_recv()
    red_pair2 = red_link[...] + red_next[...]
    red_last[0] = red_pair2
    lasts = [
        remote(red_last.at[0, pl.ds(i * n_part, n_part)], red_last.at[1, pl.ds(i * n_part, n_part)],
               red_send.at[3 + i], red_recv.at[3 + i], (y_next, x_next)[i])
        for i in range(2)
    ]
    for m in lasts:
        m.start()
    for m in lasts:
        m.wait_recv()
    red_out[pl.ds(mine, n_half), :] = red_last[0] + red_last[1]
    ref = red_out.at[pl.ds(mine, n_half)]
    back = remote(ref, ref, red_send.at[5], red_recv.at[5], pair)
    back.start()
    small_move(2).wait_recv()
    small[3, share, :] = small[2, share, :] + small_in[2, share, :]
    small_back = remote(small.at[3, share], small.at[3, share], small_send.at[3], small_recv.at[3], pair)
    small_back.start()
    remote(small.at[3, others], small.at[3, others], small_send.at[3], small_recv.at[3], pair).wait_recv()
    ref_in = red_out.at[pl.ds(other, n_half)]
    remote(ref_in, ref_in, red_send.at[5], red_recv.at[5], pair).wait_recv()

    out[0:256, :] = red_out[...]
    out[256:336, :] = small[3, 0:80, :]
    out[336:352, :] = small[3, 80:96, :] / total

    move.wait_send()
    for m in moves + lasts + [back, small_back]:
        m.wait_send()
    for i in range(3):
        count_move(i).wait_send()
        small_move(i).wait_send()
    for ph, buf in ((0, feats_all), (1, aggs_all)):
        for to in range(2, 16):
            for e in range(2):
                send_piece(ph, buf, to, e, to, pair).wait_send()
    for u in range(12):
        chip_move(u).wait_send()
    for relay in relays:
        relay.wait_send()


def _finish(sums, out_loss, out_one, out_two):
    classes = out_two.shape[0]
    out_one[...] = sums[0:256, :].T
    out_two[:, 0:128] = sums[256:256 + classes, :]
    out_two[:, 128:256] = sums[256 + classes:256 + 2 * classes, :]
    out_loss[...] = sums[336:337, 0:1]


def solution(mesh):
    def step(adj, feat, w_one, w_two, labels, mask):
        rows, nodes = adj.shape
        feat_dim, hidden = w_one.shape
        classes = w_two.shape[1]
        parts = nodes // rows
        any_spec = pl.BlockSpec(memory_space=pltpu.HBM)
        vmem = pl.BlockSpec(memory_space=pltpu.VMEM)
        quarter = rows // 4
        scratch = [
            pltpu.VMEM((parts, rows, feat_dim), BF16),
            pltpu.VMEM((parts, rows, feat_dim), BF16),
            pltpu.VMEM((rows // 2, hidden), BF16),
            pltpu.VMEM((rows // 2, hidden), BF16),
            pltpu.VMEM((rows, feat_dim), F32),
            pltpu.VMEM((rows, hidden), F32),
            pltpu.VMEM((rows, hidden), BF16),
            pltpu.VMEM((hidden, rows), BF16),
            pltpu.VMEM((128, rows), BF16),
            pltpu.VMEM((hidden, rows), F32),
            pltpu.VMEM((2, hidden, quarter), F32),
            pltpu.VMEM((4, hidden, quarter), F32),
            pltpu.VMEM((4, hidden, quarter), F32),
            pltpu.VMEM((4, hidden, quarter), F32),
            pltpu.VMEM((12, hidden, quarter), BF16),
            pltpu.VMEM((2, 8, hidden, quarter), BF16),
            pltpu.VMEM((SLOTS + 4, rows, rows // 2), BF16),
            pltpu.VMEM((feat_dim, hidden), F32),
            pltpu.VMEM((classes, hidden), F32),
            pltpu.VMEM((feat_dim, hidden), BF16),
            pltpu.VMEM((hidden, feat_dim), BF16),
            pltpu.VMEM((hidden, 128), BF16),
            pltpu.VMEM((128, hidden), BF16),
            pltpu.VMEM((1, rows), jnp.int32),
            pltpu.VMEM((1, rows), jnp.int32),
            pltpu.VMEM((3, 8, 128), F32),
            pltpu.VMEM((3, 8, 128), F32),
            pltpu.VMEM((256, 128), F32),
            pltpu.VMEM((128, 128), F32),
            pltpu.VMEM((128, 128), F32),
            pltpu.VMEM((128, 128), F32),
            pltpu.VMEM((2, 128, 128), F32),
            pltpu.VMEM((256, 128), F32),
            pltpu.VMEM((4, 96, 128), F32),
            pltpu.VMEM((3, 96, 128), F32),
            pltpu.SemaphoreType.DMA((SLOTS + 4, 2)),
            pltpu.SemaphoreType.DMA((5,)),
            pltpu.SemaphoreType.DMA((2, 32)),
            pltpu.SemaphoreType.DMA((2, 32)),
            pltpu.SemaphoreType.DMA((3,)),
            pltpu.SemaphoreType.DMA((3,)),
            pltpu.SemaphoreType.DMA((4,)),
            pltpu.SemaphoreType.DMA((16,)),
            pltpu.SemaphoreType.REGULAR,
            pltpu.SemaphoreType.DMA((12,)),
            pltpu.SemaphoreType.DMA((2, 8)),
            pltpu.SemaphoreType.DMA((6,)),
            pltpu.SemaphoreType.DMA((6,)),
            pltpu.SemaphoreType.DMA((4,)),
            pltpu.SemaphoreType.DMA((4,)),
            pltpu.SemaphoreType.DMA((2, 2)),
        ]
        sums = pl.pallas_call(
            _kernel,
            out_shape=jax.ShapeDtypeStruct((352, 128), F32),
            in_specs=[any_spec] * 6,
            out_specs=vmem,
            scratch_shapes=scratch,
            compiler_params=pltpu.CompilerParams(
                collective_id=0, has_side_effects=True, vmem_limit_bytes=67_000_000),
            name="gcn_step",
        )(adj, feat, w_one, w_two.T, labels.reshape(1, rows), mask.reshape(1, rows))
        loss, dw_one, dw_two_t = pl.pallas_call(
            _finish,
            out_shape=(
                jax.ShapeDtypeStruct((1, 1), F32),
                jax.ShapeDtypeStruct((feat_dim, hidden), F32),
                jax.ShapeDtypeStruct((classes, hidden), F32),
            ),
            in_specs=[vmem],
            out_specs=(vmem, vmem, vmem),
            name="gcn_finish",
        )(sums)
        return loss.reshape(1), dw_one, dw_two_t.T

    return jax.shard_map(
        step,
        mesh=mesh,
        in_specs=(P(AXIS, None), P(AXIS, None), P(None, None), P(None, None), P(AXIS), P(AXIS)),
        out_specs=(P(None), P(None, None), P(None, None)),
        check_vma=False,
    )
```
